32 devices in a mesh: occ: 4 (over y, core), vir: 8 (over z, x).
Axes of the slice: x: 2, y: 2, z: 4, core: 2. Of those that a mesh axis runs over, the one named last changes fastest.
Arguments:
- amplitudes: bfloat16 [2048, 4096], P('occ', 'vir'), may hold values from -6 to 6
- hole_integrals: bfloat16 [2048, 2048], P('occ'), may hold values from -0.375 to 0.375
- particle_integrals: bfloat16 [4096, 4096], P('vir'), may hold values from -0.375 to 0.375
- occ_irrep: int32 [32], replicated, may hold values from 0 to 7
- vir_irrep: int32 [64], replicated, may hold values from 0 to 7
- occ_energy: float32 [2048], P('occ'), may hold values from -1.5 to -0.5
- vir_energy: float32 [4096], P('vir'), may hold values from 0.5 to 2.5
Outputs:
- update: float32 [4096, 2048], P('vir', 'occ')
The draws below stay inside these ranges and needn't reach their ends.
All inputs are finite; a program needn't handle non-finite values.
Results may differ from the reference program's by a relative error of at most 0.0003.
Values may be sent and summed in bfloat16 or wider, within the bound.
A program may use at most 128 MiB of HBM per device.

```python
import jax
import jax.numpy as jnp

TILE = 64
P_SIZE = 2048
Q = 4096


def with_ends(array, own_key, low, top_value):
    spot = [jax.random.randint(jax.random.fold_in(own_key, axis), (), 0, length) for axis, length in enumerate(array.shape)]
    widest = array.shape.index(max(array.shape))
    neighbour = spot[:widest] + [(spot[widest] + 1) % array.shape[widest]] + spot[widest + 1:]
    return array.at[tuple(spot)].set(low).at[tuple(neighbour)].set(top_value)


def with_spikes(entries, key, source, target, blocks, factor):
    owner, partner = [(jnp.arange(entries.shape[position]) // (entries.shape[position] // blocks)).reshape([-1 if axis == position else 1 for axis in range(entries.ndim)]) for position in (source, target)]
    chosen = jax.random.permutation(key, blocks)[partner]
    strong = (owner == chosen) | (owner == (partner + blocks // 2) % blocks)
    return jnp.where(strong, factor * entries, entries)


def steps_of(stream_key, extent, shards, low, top_value):
    gain = 1.0
    for dim, blocks in shards:
        steps = jax.random.uniform(jax.random.fold_in(jax.random.fold_in(stream_key, 6), dim), (blocks,), jnp.float32, low / len(shards), top_value / len(shards))
        gain = gain * jnp.repeat(jnp.exp(steps), extent[dim] // blocks).reshape((-1,) + (1,) * (len(extent) - 1 - dim))
    return gain


def gaussian(stream_key, dims, width, limit, split=(), dtype=jnp.bfloat16):
    result = jax.random.normal(stream_key, dims, jnp.float32) * width
    if len(split) > 0:
        result = steps_of(stream_key, dims, split, -0.22, 0.18) * result
    return jnp.clip(result, min=-limit, max=limit).astype(dtype)


def heavy_noise(stream_key, shape, spread, most, pieces, heavy, dtype=jnp.bfloat16):
    result = spread * jax.random.normal(stream_key, shape, jnp.float32)
    if pieces:
        result = result * steps_of(stream_key, shape, pieces, -0.22, 0.18)
    return jnp.clip(with_spikes(result, jax.random.fold_in(stream_key, 3), *heavy), -most, most).astype(dtype)


def setup_inputs(seed: int = 0) -> dict:
    keys = jax.random.split(jax.random.key(seed), 8)
    amplitudes = gaussian(keys[0], (P_SIZE, Q), 1.0, 6.0, ((0, 4), (1, 8)))
    hole_integrals = gaussian(keys[1], (P_SIZE, P_SIZE), (P_SIZE // 8) ** -0.5, 0.375, ((0, 4),))
    particle_integrals = heavy_noise(keys[2], (Q, Q), (Q // 8) ** -0.5, 0.375, ((0, 8),), (0, 1, 8, 2.0))
    occ_irrep = with_ends(jax.random.randint(keys[3], (P_SIZE // TILE,), 0, 8), jax.random.fold_in(keys[3], 1), 0, 7).astype(jnp.int32)
    vir_irrep = with_ends(jax.random.randint(keys[4], (Q // TILE,), 0, 8), jax.random.fold_in(keys[4], 1), 0, 7).astype(jnp.int32)
    occ_energy = jnp.clip(-1.5 + 1.0 * jax.random.uniform(keys[5], (P_SIZE,), jnp.float32) ** steps_of(keys[5], (P_SIZE,), ((0, 4),), -0.2, 0.2), -1.5, -0.5)
    vir_energy = jnp.clip(0.5 + 2.0 * jax.random.uniform(keys[6], (Q,), jnp.float32) ** steps_of(keys[6], (Q,), ((0, 8),), -0.2, 0.2), 0.5, 2.5)
    return {"amplitudes": amplitudes, "hole_integrals": hole_integrals, "particle_integrals": particle_integrals, "occ_irrep": occ_irrep, "vir_irrep": vir_irrep, "occ_energy": occ_energy, "vir_energy": vir_energy}


def reference(amplitudes, hole_integrals, particle_integrals, occ_irrep, vir_irrep, occ_energy, vir_energy):
    occ_labels = jnp.repeat(occ_irrep, TILE)
    vir_labels = jnp.repeat(vir_irrep, TILE)
    zero_value = jnp.zeros((), jnp.bfloat16)
    hole_masked = jnp.where(occ_labels[:, None] == occ_labels[None, :], hole_integrals, zero_value)
    particle_masked = jnp.where(vir_labels[:, None] == vir_labels[None, :], particle_integrals, zero_value)
    hole = jnp.dot(hole_masked, amplitudes, preferred_element_type=jnp.float32)
    particle = jnp.dot(amplitudes, particle_masked, preferred_element_type=jnp.float32)
    energy_gap = vir_energy[:, None] - occ_energy[None, :]
    return (hole + particle).T / energy_gap
```

```python
import functools

import jax
import jax.numpy as jnp
from jax import lax
from jax.experimental import pallas as pl
from jax.experimental.pallas import tpu as pltpu
from jax.sharding import PartitionSpec as P

TILE = 64
CORES = 2
LINES = 4
ROWS = 4
HALVES = 2
TOP = 32000.0
MESH = pl.DeviceIdType.MESH
ORDER = (
    ("t", 0), ("v", 0, 0), ("v", 0, 1), ("t", 1), ("v", 1, 0), ("t", 2), ("t", 3), ("v", 1, 1),
    ("v", 2, 0), ("v", 2, 1), ("v", 3, 0), ("v", 3, 1),
)


def kernel(
    width, groups, amp, hole, slab, occ_irrep, vir_irrep, occ_e, vir_e, out,
    occ_tags, vir_tags, occ_labels, vir_labels, occ_row, vir_row,
    t_all, v_all, v_masked, v_send, cols_all, hole_all, acc, tmp, box_out, scale_out, box_in, scale_in, result,
    t_send, t_sem, v_sends, v_sem, relay_send, pair_send, pair_sem,
    box_send, box_sem, scale_send, scale_sem, local_sem, own_sem, load_sem, out_sem,
):
    p_own, q_own = amp.shape
    o, v = lax.axis_index("occ"), lax.axis_index("vir")
    c = lax.rem(o, CORES)
    z, x = v // width, lax.rem(v, width)
    occ_size = groups * CORES
    partner = o + 1 - 2 * c
    half = z // 2
    mid = lax.rem(z + half, 2)
    mate, far, near = z + 1 - 2 * lax.rem(z, 2), 3 * (1 - half), 2 - half
    owner = [mid * mate + (1 - mid) * far, mid * far + (1 - mid) * near, mid * near + (1 - mid) * mate, z]
    target = [mate, mid * far + (1 - mid) * mate, mid * near + (1 - mid) * mate]
    box = [2 * (1 - mid), mid + 3 * (1 - mid), mid]
    is_mid = mid == 1
    rows, cols, share = p_own // ROWS, q_own // HALVES, q_own // CORES
    tiles = q_own // TILE
    others = range(1, width)

    def xdev(k):
        return (o, z * width + lax.rem(x + k, width))

    def remote(src, dst, send, recv, device):
        return pltpu.make_async_remote_copy(
            src_ref=src, dst_ref=dst, send_sem=send, recv_sem=recv, device_id=device, device_id_type=MESH
        )

    def landed(ref, sem):
        pltpu.make_async_copy(ref, ref, sem).wait()

    barrier = pltpu.get_barrier_semaphore()
    peers = [(lax.rem(o + d, occ_size), v) for d in range(1, occ_size)]
    peers += [xdev(k) for k in others] + [(o, mate * width + x), (o, near * width + x)]
    for peer in peers:
        pl.semaphore_signal(barrier, inc=1, device_id=peer, device_id_type=MESH)

    loads = {}

    def load(name, src, dst, sem):
        loads[name] = pltpu.make_async_copy(src, dst, sem)
        loads[name].start()

    def columns(zz, xx):
        return pl.ds(pl.multiple_of((zz * width + xx) * q_own, q_own), q_own)

    load("amp", amp, t_all.at[:, pl.ds(0, q_own)], load_sem.at[0])
    for j in range(LINES):
        for k in others:
            load(
                ("send", j, k),
                slab.at[pl.ds(pl.multiple_of(c * share, share), share), columns(owner[j], lax.rem(x + k, width))],
                v_send.at[j, k - 1], local_sem.at[j, k - 1],
            )
        load(("own", j), slab.at[:, columns(owner[j], x)], v_all.at[j, pl.ds(0, q_own), :], own_sem.at[j])
    load("occ_tags", occ_irrep, occ_tags, load_sem.at[1])
    load("vir_tags", vir_irrep, vir_tags, load_sem.at[2])
    load("occ_row", occ_e, occ_row, load_sem.at[3])
    load("vir_row", vir_e, vir_row, load_sem.at[4])
    load("hole", hole, hole_all, load_sem.at[5])

    pl.semaphore_wait(barrier, len(peers) - 1 + 2 * mid)

    def t_copy(i, k):
        at = pl.ds(i * rows, rows)
        return remote(
            t_all.at[at, pl.ds(0, q_own)], t_all.at[at, pl.ds((width - k) * q_own, q_own)],
            t_send.at[k - 1, i], t_sem.at[width - k - 1, i], xdev(k),
        )

    def v_piece(j, h, d, core):
        return v_all.at[
            j, pl.ds(pl.multiple_of(d * q_own + core * share, share), share), pl.ds(h * cols, cols)
        ]

    def v_copy(j, h, k):
        return remote(
            v_send.at[j, k - 1, :, pl.ds(h * cols, cols)], v_piece(j, h, width - k, c),
            v_sends.at[k - 1, j, h], v_sem.at[width - k - 1, j, h, c], xdev(k),
        )

    def relay_copy(j, h, d):
        piece = v_piece(j, h, d, c)
        return remote(piece, piece, relay_send.at[d - 1, j, h], v_sem.at[d - 1, j, h, c], (partner, v))

    def pair_copy(d):
        return remote(
            t_all.at[:, pl.ds(0, q_own)], cols_all.at[pl.ds(pl.multiple_of(o * p_own, p_own), p_own), :],
            pair_send.at[d - 1], pair_sem.at[o], (lax.rem(o + d, occ_size), v),
        )

    loads["amp"].wait()
    fetched = set()
    for step in ORDER:
        if step[0] == "t":
            for k in others:
                t_copy(step[1], k).start()
            if step[1] == 0:
                for d in range(1, occ_size):
                    pair_copy(d).start()
                load("pairs", amp, cols_all.at[pl.ds(pl.multiple_of(o * p_own, p_own), p_own), :], load_sem.at[6])
        else:
            for k in others:
                if (step[1], k) not in fetched:
                    fetched.add((step[1], k))
                    loads["send", step[1], k].wait()
                v_copy(step[1], step[2], k).start()

    loads["occ_tags"].wait()
    loads["vir_tags"].wait()
    low = lax.broadcasted_iota(jnp.int32, (1, 2 * TILE), 1) < TILE
    for j in range(LINES):
        base = (owner[j] * width + x) * tiles

        @pl.loop(0, tiles // 2)
        def _(i):
            at = pl.ds(pl.multiple_of(i * 2 * TILE, 2 * TILE), 2 * TILE)
            vir_labels[j, :, at] = jnp.where(low, vir_tags[base + 2 * i], vir_tags[base + 2 * i + 1])

    @pl.loop(0, occ_tags.shape[0] // 2)
    def _(i):
        at = pl.ds(pl.multiple_of(i * 2 * TILE, 2 * TILE), 2 * TILE)
        occ_labels[:, at] = jnp.where(low, occ_tags[2 * i], occ_tags[2 * i + 1])

    def mask(j, d, at):
        first = (z * width + lax.rem(x + d, width)) * tiles
        labels = vir_labels[j, :, at]

        @pl.loop(0, tiles)
        def _(i):
            part = pl.ds(pl.multiple_of(d * q_own + i * TILE, TILE), TILE)
            keep = (labels == vir_tags[first + i]).astype(jnp.float32).astype(jnp.bfloat16)
            v_masked[j, part, at] = v_all[j, part, at] * keep

    everything = pl.ds(0, q_own)
    loads["own", 0].wait()
    mask(0, 0, everything)

    loads["hole"].wait()

    @pl.loop(0, p_own // TILE)
    def _(i):
        at = pl.ds(pl.multiple_of(i * TILE, TILE), TILE)
        keep = (occ_labels[...] == occ_tags[o * (p_own // TILE) + i]).astype(jnp.float32).astype(jnp.bfloat16)
        hole_all[at, :] = hole_all[at, :] * keep

    def box_copies(j, h, i):
        at, there = pl.ds(pl.multiple_of(i * rows, rows), rows), pl.ds(h * cols, cols)
        device = (o, target[j] * width + x)
        return (
            remote(
                box_out.at[j, at, there], box_in.at[box[j], at, there],
                box_send.at[j, h, i], box_sem.at[box[j], h, i], device,
            ),
            remote(
                scale_out.at[j * ROWS + i, :, there], scale_in.at[box[j] * ROWS + i, :, there],
                scale_send.at[j, h, i], scale_sem.at[box[j], h, i], device,
            ),
        )

    def arrived(b, h, i):
        at, there = pl.ds(pl.multiple_of(i * rows, rows), rows), pl.ds(h * cols, cols)
        landed(box_in.at[b, at, there], box_sem.at[b, h, i])
        landed(scale_in.at[b * ROWS + i, :, there], scale_sem.at[b, h, i])
        return box_in[b, at, there].astype(jnp.float32) * scale_in[b * ROWS + i, :, there]

    def unit(j, h, i):
        at, there = pl.ds(pl.multiple_of(i * rows, rows), rows), pl.ds(h * cols, cols)
        part = jnp.dot(t_all[at, :], v_masked[j, :, there], preferred_element_type=jnp.float32)
        if j == LINES - 1:
            acc[at, there] += part
            return
        if j > 0:
            tmp[...] = part

            @pl.when(is_mid)
            def _():
                tmp[...] += arrived(j + 1, h, i)

            part = tmp[...]
        most = jnp.maximum(jnp.max(jnp.abs(part), axis=0, keepdims=True), 1e-30)
        box_out[j, at, there] = jnp.round(part * (TOP / most)).astype(jnp.int32).astype(jnp.int16)
        scale_out[j * ROWS + i, :, there] = most * (1.0 / TOP)
        for copy in box_copies(j, h, i):
            copy.start()

    have_t, have_v = 0, []
    for step in ORDER:
        if step[0] == "t":
            i = step[1]
            for d in others:
                landed(t_all.at[pl.ds(i * rows, rows), pl.ds(d * q_own, q_own)], t_sem.at[d - 1, i])
            have_t = i + 1
            for j, h in have_v:
                unit(j, h, i)
        else:
            j, h = step[1:]
            for d in others:
                landed(v_piece(j, h, d, c), v_sem.at[d - 1, j, h, c])
                relay_copy(j, h, d).start()
            if h == 0 and j > 0:
                loads["own", j].wait()
                mask(j, 0, everything)
            if j == LINES - 1 and h == 0:
                loads["pairs"].wait()
                for d in range(1, occ_size):
                    oo = lax.rem(o + d, occ_size)
                    landed(cols_all.at[pl.ds(pl.multiple_of(oo * p_own, p_own), p_own), :], pair_sem.at[oo])

                @pl.loop(0, ROWS)
                def _(i):
                    at = pl.ds(pl.multiple_of(i * rows, rows), rows)
                    acc[at, :] = jnp.dot(hole_all[at, :], cols_all[...], preferred_element_type=jnp.float32)

            for d in others:
                landed(v_piece(j, h, d, 1 - c), v_sem.at[d - 1, j, h, 1 - c])
                mask(j, d, pl.ds(h * cols, cols))
            have_v.append((j, h))
            if have_t == ROWS:

                @pl.loop(0, ROWS)
                def _(i):
                    unit(j, h, i)
            else:
                for i in range(have_t):
                    unit(j, h, i)

    loads["occ_row"].wait()
    loads["vir_row"].wait()

    def out_copy(h, i):
        at, there = pl.ds(pl.multiple_of(i * rows, rows), rows), pl.ds(h * cols, cols)
        return pltpu.make_async_copy(result.at[there, at], out.at[there, at], out_sem.at[h, i])

    for h in range(HALVES):
        there = pl.ds(h * cols, cols)
        column = jnp.broadcast_to(vir_row[:, there], (rows, cols)).T

        @pl.loop(0, ROWS)
        def _(i):
            at = pl.ds(pl.multiple_of(i * rows, rows), rows)
            total = acc[at, there] + arrived(1, h, i)
            total = total + arrived(0, h, i)
            result[there, at] = total.T / (column - occ_row[:, at])
            out_copy(h, i).start()

    for h in range(HALVES):

        @pl.loop(0, ROWS)
        def _(i):
            out_copy(h, i).wait()
            for j in range(LINES - 1):
                for copy in box_copies(j, h, i):
                    copy.wait_send()

    for d in range(1, occ_size):
        pair_copy(d).wait_send()
    for k in others:
        for i in range(ROWS):
            t_copy(i, k).wait_send()
        for j in range(LINES):
            for h in range(HALVES):
                v_copy(j, h, k).wait_send()
                relay_copy(j, h, k).wait_send()


def per_device(
    occ_size, vir_size, amplitudes, hole_integrals, particle_integrals, occ_irrep, vir_irrep, occ_energy, vir_energy
):
    width, groups = vir_size // LINES, occ_size // CORES
    p_own, q_own = amplitudes.shape
    p_all = p_own * occ_size
    bf16, f32, i32 = jnp.bfloat16, jnp.float32, jnp.int32
    dma = pltpu.SemaphoreType.DMA
    anywhere = pl.BlockSpec(memory_space=pl.ANY)
    return pl.pallas_call(
        functools.partial(kernel, width, groups),
        out_shape=jax.ShapeDtypeStruct((q_own, p_own), f32),
        in_specs=[anywhere] * 7,
        out_specs=anywhere,
        scratch_shapes=[
            pltpu.SMEM(occ_irrep.shape, i32),
            pltpu.SMEM(vir_irrep.shape, i32),
            pltpu.VMEM((1, p_all), i32),
            pltpu.VMEM((LINES, 1, q_own), i32),
            pltpu.VMEM((1, p_own), f32),
            pltpu.VMEM((1, q_own), f32),
            pltpu.VMEM((p_own, width * q_own), bf16),
            pltpu.VMEM((LINES, width * q_own, q_own), bf16),
            pltpu.VMEM((LINES, width * q_own, q_own), bf16),
            pltpu.VMEM((LINES, width - 1, q_own // CORES, q_own), bf16),
            pltpu.VMEM((p_all, q_own), bf16),
            pltpu.VMEM((p_own, p_all), bf16),
            pltpu.VMEM((p_own, q_own), f32),
            pltpu.VMEM((p_own // ROWS, q_own // HALVES), f32),
            pltpu.VMEM((LINES - 1, p_own, q_own), jnp.int16),
            pltpu.VMEM(((LINES - 1) * ROWS, 1, q_own), f32),
            pltpu.VMEM((LINES, p_own, q_own), jnp.int16),
            pltpu.VMEM((LINES * ROWS, 1, q_own), f32),
            pltpu.VMEM((q_own, p_own), f32),
            dma((width - 1, ROWS)),
            dma((width - 1, ROWS)),
            dma((width - 1, LINES, HALVES)),
            dma((width - 1, LINES, HALVES, CORES)),
            dma((width - 1, LINES, HALVES)),
            dma((occ_size - 1,)),
            dma((occ_size,)),
            dma((LINES - 1, HALVES, ROWS)),
            dma((LINES, HALVES, ROWS)),
            dma((LINES - 1, HALVES, ROWS)),
            dma((LINES, HALVES, ROWS)),
            dma((LINES, width - 1)),
            dma((LINES,)),
            dma((7,)),
            dma((HALVES, ROWS)),
        ],
        compiler_params=pltpu.CompilerParams(
            collective_id=0, has_side_effects=True, vmem_limit_bytes=60 * 1024 * 1024
        ),
    )(
        amplitudes, hole_integrals, particle_integrals, occ_irrep, vir_irrep,
        occ_energy[None, :], vir_energy[None, :],
    )


def solution(mesh):
    placed = (P("occ", "vir"), P("occ", None), P("vir", None), P(), P(), P("occ"), P("vir"))
    return jax.shard_map(
        functools.partial(per_device, mesh.shape["occ"], mesh.shape["vir"]),
        mesh=mesh, in_specs=placed, out_specs=P("vir", "occ"), check_vma=False,
    )
```

```python
import functools

import jax
import jax.numpy as jnp
from jax import lax
from jax.experimental import pallas as pl
from jax.experimental.pallas import tpu as pltpu
from jax.sharding import PartitionSpec as P

TILE = 64
CORES = 2
LINES = 4
ROWS = 4
HALVES = 2
EARLY = 1
TOP = 32000.0
MESH = pl.DeviceIdType.MESH
ORDER = "ttvvttvvvv"


def kernel(
    width, groups, amp, hole, slab, occ_irrep, vir_irrep, occ_e, vir_e, out,
    occ_tags, vir_tags, occ_labels, vir_labels, occ_row, vir_row,
    t_all, v_all, v_masked, v_send, v_mate, cols_all, hole_all, acc, tmp, box_out, scale_out, box_in, scale_in, result,
    mate_labels, early_out, early_scale_out, early_in, early_scale_in, extra_in, extra_scale_in,
    t_send, t_sem, v_sends, v_sem, relay_send, pair_send, pair_sem,
    box_send, box_sem, scale_send, scale_sem, local_sem, own_sem, load_sem, out_sem,
    mate_load, early_send, early_sem, extra_send, extra_sem,
):
    p_own, q_own = amp.shape
    o, v = lax.axis_index("occ"), lax.axis_index("vir")
    c = lax.rem(o, CORES)
    z, x = v // width, lax.rem(v, width)
    occ_size = groups * CORES
    partner = o + 1 - 2 * c
    half = z // 2
    mid = lax.rem(z + half, 2)
    mate, far, near = z + 1 - 2 * lax.rem(z, 2), 3 * (1 - half), 2 - half
    owner = [far, mid * mate + (1 - mid) * near, mid * near + (1 - mid) * mate, z]
    target = [mid * far + (1 - mid) * mate, mate, mid * near + (1 - mid) * mate]
    box = [2 - mid, 3 * (1 - mid), mid]
    is_mid = mid == 1
    rows, cols, share = p_own // ROWS, q_own // HALVES, q_own // CORES
    tiles = q_own // TILE
    others = range(1, width)
    early = pl.ds(0, EARLY * rows)
    order, count = [], {"t": 0, "v": 0}
    for kind in ORDER + "v" * HALVES:
        order.append((kind, count[kind]) if kind == "t" else (kind, count[kind] // HALVES, count[kind] % HALVES))
        count[kind] += 1

    def xdev(k):
        return (o, z * width + lax.rem(x + k, width))

    def remote(src, dst, send, recv, device):
        return pltpu.make_async_remote_copy(
            src_ref=src, dst_ref=dst, send_sem=send, recv_sem=recv, device_id=device, device_id_type=MESH
        )

    def landed(ref, sem):
        pltpu.make_async_copy(ref, ref, sem).wait()

    barrier = pltpu.get_barrier_semaphore()
    peers = [(lax.rem(o + d, occ_size), v) for d in range(1, occ_size)]
    peers += [xdev(k) for k in others] + [(o, mate * width + x), (o, near * width + x)]
    for peer in peers:
        pl.semaphore_signal(barrier, inc=1, device_id=peer, device_id_type=MESH)

    loads = {}

    def load(name, src, dst, sem):
        loads[name] = pltpu.make_async_copy(src, dst, sem)
        loads[name].start()

    def columns(zz, xx):
        return pl.ds(pl.multiple_of((zz * width + xx) * q_own, q_own), q_own)

    load("amp", amp, t_all.at[:, pl.ds(0, q_own)], load_sem.at[0])
    load("occ_tags", occ_irrep, occ_tags, load_sem.at[1])
    load("vir_tags", vir_irrep, vir_tags, load_sem.at[2])
    for k in range(width):
        load(("mate", k), slab.at[:, columns(mate, lax.rem(x + k, width))], v_mate.at[k], mate_load.at[k])
    for j in range(LINES):
        for k in others:
            load(
                ("send", j, k),
                slab.at[pl.ds(pl.multiple_of(c * share, share), share), columns(owner[j], lax.rem(x + k, width))],
                v_send.at[j, k - 1], local_sem.at[j, k - 1],
            )
        load(("own", j), slab.at[:, columns(owner[j], x)], v_all.at[j, pl.ds(0, q_own), :], own_sem.at[j])
    load("occ_row", occ_e, occ_row, load_sem.at[3])
    load("vir_row", vir_e, vir_row, load_sem.at[4])
    load("hole", hole, hole_all, load_sem.at[5])

    pl.semaphore_wait(barrier, len(peers) - 1 + 2 * mid)

    def t_copy(i, k):
        at = pl.ds(i * rows, rows)
        return remote(
            t_all.at[at, pl.ds(0, q_own)], t_all.at[at, pl.ds((width - k) * q_own, q_own)],
            t_send.at[k - 1, i], t_sem.at[width - k - 1, i], xdev(k),
        )

    def v_piece(j, h, d, core):
        return v_all.at[
            j, pl.ds(pl.multiple_of(d * q_own + core * share, share), share), pl.ds(h * cols, cols)
        ]

    def v_copy(j, h, k):
        return remote(
            v_send.at[j, k - 1, :, pl.ds(h * cols, cols)], v_piece(j, h, width - k, c),
            v_sends.at[k - 1, j, h], v_sem.at[width - k - 1, j, h, c], xdev(k),
        )

    def relay_copy(j, h, d):
        piece = v_piece(j, h, d, c)
        return remote(piece, piece, relay_send.at[d - 1, j, h], v_sem.at[d - 1, j, h, c], (partner, v))

    def pair_copy(d):
        return remote(
            t_all.at[:, pl.ds(0, q_own)], cols_all.at[pl.ds(pl.multiple_of(o * p_own, p_own), p_own), :],
            pair_send.at[d - 1], pair_sem.at[o], (lax.rem(o + d, occ_size), v),
        )

    fetched = set()

    def x_send(step):
        for k in others:
            if step[0] == "t":
                t_copy(step[1], k).start()
                continue
            if (step[1], k) not in fetched:
                fetched.add((step[1], k))
                loads["send", step[1], k].wait()
            v_copy(step[1], step[2], k).start()

    loads["amp"].wait()
    for step in order[:-HALVES]:
        x_send(step)
        if step == ("t", 0):
            for d in range(1, occ_size):
                pair_copy(d).start()
            load("pairs", amp, cols_all.at[pl.ds(pl.multiple_of(o * p_own, p_own), p_own), :], load_sem.at[6])

    loads["occ_tags"].wait()
    loads["vir_tags"].wait()
    low = lax.broadcasted_iota(jnp.int32, (1, 2 * TILE), 1) < TILE

    def label(ref, j, zz, xx):
        base = (zz * width + xx) * tiles

        @pl.loop(0, tiles // 2)
        def _(i):
            at = pl.ds(pl.multiple_of(i * 2 * TILE, 2 * TILE), 2 * TILE)
            ref[j, :, at] = jnp.where(low, vir_tags[base + 2 * i], vir_tags[base + 2 * i + 1])

    def pack(part):
        most = jnp.maximum(jnp.max(jnp.abs(part), axis=0, keepdims=True), 1e-30)
        return jnp.round(part * (TOP / most)).astype(jnp.int32).astype(jnp.int16), most * (1.0 / TOP)

    def early_copies(k):
        land, where = (box_in.at[0, early, :], scale_in.at[0]) if k == 0 else (early_in.at[k - 1], early_scale_in.at[k - 1])
        device = (o, mate * width + x)
        return (
            remote(early_out.at[k], land, early_send.at[0, k], early_sem.at[0, k], device),
            remote(early_scale_out.at[k], where, early_send.at[1, k], early_sem.at[1, k], device),
        )

    def extra_copies(k):
        return (
            remote(early_in.at[k - 1], extra_in.at[width - k - 1], extra_send.at[0, k - 1], extra_sem.at[0, width - k - 1], xdev(k)),
            remote(
                early_scale_in.at[k - 1], extra_scale_in.at[width - k - 1],
                extra_send.at[1, k - 1], extra_sem.at[1, width - k - 1], xdev(k),
            ),
        )

    for k in reversed(range(width)):
        label(mate_labels, k, mate, lax.rem(x + k, width))
        loads["mate", k].wait()

        @pl.loop(0, tiles)
        def _(i):
            part = pl.ds(pl.multiple_of(i * TILE, TILE), TILE)
            keep = (mate_labels[k] == vir_tags[(z * width + x) * tiles + i]).astype(jnp.float32).astype(jnp.bfloat16)
            v_mate[k, part, :] = v_mate[k, part, :] * keep

        early_out[k], early_scale_out[k] = pack(
            jnp.dot(t_all[early, pl.ds(0, q_own)], v_mate[k], preferred_element_type=jnp.float32)
        )
        for copy in early_copies(k):
            copy.start()

    for j in range(LINES):
        label(vir_labels, j, owner[j], x)

    @pl.loop(0, occ_tags.shape[0] // 2)
    def _(i):
        at = pl.ds(pl.multiple_of(i * 2 * TILE, 2 * TILE), 2 * TILE)
        occ_labels[:, at] = jnp.where(low, occ_tags[2 * i], occ_tags[2 * i + 1])

    def mask(j, d, at):
        first = (z * width + lax.rem(x + d, width)) * tiles
        labels = vir_labels[j, :, at]

        @pl.loop(0, tiles)
        def _(i):
            part = pl.ds(pl.multiple_of(d * q_own + i * TILE, TILE), TILE)
            keep = (labels == vir_tags[first + i]).astype(jnp.float32).astype(jnp.bfloat16)
            v_masked[j, part, at] = v_all[j, part, at] * keep

    everything = pl.ds(0, q_own)
    loads["own", 0].wait()
    mask(0, 0, everything)

    loads["hole"].wait()

    @pl.loop(0, p_own // TILE)
    def _(i):
        at = pl.ds(pl.multiple_of(i * TILE, TILE), TILE)
        keep = (occ_labels[...] == occ_tags[o * (p_own // TILE) + i]).astype(jnp.float32).astype(jnp.bfloat16)
        hole_all[at, :] = hole_all[at, :] * keep

    def box_copies(j, h, i):
        at, there = pl.ds(pl.multiple_of(i * rows, rows), rows), pl.ds(h * cols, cols)
        device = (o, target[j] * width + x)
        return (
            remote(
                box_out.at[j, at, there], box_in.at[box[j], at, there],
                box_send.at[j, h, i], box_sem.at[box[j], h, i], device,
            ),
            remote(
                scale_out.at[j * ROWS + i, :, there], scale_in.at[box[j] * ROWS + i, :, there],
                scale_send.at[j, h, i], scale_sem.at[box[j], h, i], device,
            ),
        )

    def arrived(b, h, i):
        at, there = pl.ds(pl.multiple_of(i * rows, rows), rows), pl.ds(h * cols, cols)
        landed(box_in.at[b, at, there], box_sem.at[b, h, i])
        landed(scale_in.at[b * ROWS + i, :, there], scale_sem.at[b, h, i])
        return box_in[b, at, there].astype(jnp.float32) * scale_in[b * ROWS + i, :, there]

    def unit(j, h, i):
        at, there = pl.ds(pl.multiple_of(i * rows, rows), rows), pl.ds(h * cols, cols)

        def product():
            return jnp.dot(t_all[at, :], v_masked[j, :, there], preferred_element_type=jnp.float32)

        def send(part):
            box_out[j, at, there], scale_out[j * ROWS + i, :, there] = pack(part)
            for copy in box_copies(j, h, i):
                copy.start()

        def merge(b):
            tmp[...] = product()

            @pl.when(is_mid)
            def _():
                tmp[...] += arrived(b, h, i)

            send(tmp[...])

        if j == LINES - 1:
            acc[at, there] += product()
        elif j == 0:
            merge(2)
        elif j == 1:
            pl.when(jnp.logical_or(i >= EARLY, mid == 0))(lambda: send(product()))
        else:
            pl.when(jnp.logical_or(i >= EARLY, is_mid))(lambda: merge(3))

    have_t, have_v = 0, []
    for n, step in enumerate(order):
        if n == ORDER.rindex("t") + 1:
            for k in others:
                landed(early_in.at[k - 1], early_sem.at[0, k])
                landed(early_scale_in.at[k - 1], early_sem.at[1, k])
                for copy in extra_copies(k):
                    copy.start()
            for last in order[-HALVES:]:
                x_send(last)
        if step[0] == "t":
            i = step[1]
            for d in others:
                landed(t_all.at[pl.ds(i * rows, rows), pl.ds(d * q_own, q_own)], t_sem.at[d - 1, i])
            have_t = i + 1
            for j, h in have_v:
                unit(j, h, i)
        else:
            j, h = step[1:]
            for d in others:
                landed(v_piece(j, h, d, c), v_sem.at[d - 1, j, h, c])
                relay_copy(j, h, d).start()
            if h == 0 and j > 0:
                loads["own", j].wait()
                mask(j, 0, everything)
            if j == LINES - 1 and h == 0:
                loads["pairs"].wait()
                for d in range(1, occ_size):
                    oo = lax.rem(o + d, occ_size)
                    landed(cols_all.at[pl.ds(pl.multiple_of(oo * p_own, p_own), p_own), :], pair_sem.at[oo])

                @pl.loop(0, ROWS)
                def _(i):
                    at = pl.ds(pl.multiple_of(i * rows, rows), rows)
                    acc[at, :] = jnp.dot(hole_all[at, :], cols_all[...], preferred_element_type=jnp.float32)

            for d in others:
                landed(v_piece(j, h, d, 1 - c), v_sem.at[d - 1, j, h, 1 - c])
                mask(j, d, pl.ds(h * cols, cols))
            have_v.append((j, h))
            if have_t == ROWS:

                @pl.loop(0, ROWS)
                def _(i):
                    unit(j, h, i)
            else:
                for i in range(have_t):
                    unit(j, h, i)

    loads["occ_row"].wait()
    loads["vir_row"].wait()
    for i in range(ROWS):
        at = pl.ds(i * rows, rows)
        result[:, at] = 1.0 / (jnp.broadcast_to(vir_row[...], (rows, q_own)).T - occ_row[:, at])

    for h in range(HALVES):

        @pl.loop(0, ROWS)
        def _(i):
            at, there = pl.ds(pl.multiple_of(i * rows, rows), rows), pl.ds(h * cols, cols)
            acc[at, there] += arrived(1, h, i)

    landed(box_in.at[0, early, :], early_sem.at[0, 0])
    landed(scale_in.at[0], early_sem.at[1, 0])
    acc[early, :] += box_in[0, early, :].astype(jnp.float32) * scale_in[0]
    for d in others:
        landed(extra_in.at[d - 1], extra_sem.at[0, d - 1])
        landed(extra_scale_in.at[d - 1], extra_sem.at[1, d - 1])
        acc[early, :] += extra_in[d - 1].astype(jnp.float32) * extra_scale_in[d - 1]

    def out_copy(h, i):
        at, there = pl.ds(pl.multiple_of(i * rows, rows), rows), pl.ds(h * cols, cols)
        return pltpu.make_async_copy(result.at[there, at], out.at[there, at], out_sem.at[h, i])

    def finish(h, i, total):
        at, there = pl.ds(pl.multiple_of(i * rows, rows), rows), pl.ds(h * cols, cols)
        result[there, at] = total.T * result[there, at]
        out_copy(h, i).start()

    for h in range(HALVES):
        there = pl.ds(h * cols, cols)
        for i in range(EARLY):
            finish(h, i, acc[pl.ds(i * rows, rows), there])

        if h == HALVES - 1:
            for d in range(1, occ_size):
                pair_copy(d).wait_send()
            for k in range(width):
                for copy in early_copies(k):
                    copy.wait_send()
            for k in others:
                for copy in extra_copies(k):
                    copy.wait_send()
                for i in range(ROWS):
                    t_copy(i, k).wait_send()
                for j in range(LINES):
                    for hh in range(HALVES):
                        v_copy(j, hh, k).wait_send()
                        relay_copy(j, hh, k).wait_send()
            for j in range(LINES - 1):
                for hh in range(HALVES):

                    @pl.loop(0, ROWS)
                    def _(i):
                        @pl.when(jnp.logical_or(i >= EARLY, jnp.logical_or(j == 0, mid == j - 1)))
                        def _():
                            for copy in box_copies(j, hh, i):
                                copy.wait_send()

        @pl.loop(EARLY, ROWS)
        def _(i):
            at = pl.ds(pl.multiple_of(i * rows, rows), rows)
            finish(h, i, acc[at, there] + arrived(0, h, i))

    for h in range(HALVES):

        @pl.loop(0, ROWS)
        def _(i):
            out_copy(h, i).wait()


def per_device(
    occ_size, vir_size, amplitudes, hole_integrals, particle_integrals, occ_irrep, vir_irrep, occ_energy, vir_energy
):
    width, groups = vir_size // LINES, occ_size // CORES
    p_own, q_own = amplitudes.shape
    p_all, early = p_own * occ_size, EARLY * p_own // ROWS
    bf16, f32, i32 = jnp.bfloat16, jnp.float32, jnp.int32
    dma = pltpu.SemaphoreType.DMA
    anywhere = pl.BlockSpec(memory_space=pl.ANY)
    return pl.pallas_call(
        functools.partial(kernel, width, groups),
        out_shape=jax.ShapeDtypeStruct((q_own, p_own), f32),
        in_specs=[anywhere] * 7,
        out_specs=anywhere,
        scratch_shapes=[
            pltpu.SMEM(occ_irrep.shape, i32),
            pltpu.SMEM(vir_irrep.shape, i32),
            pltpu.VMEM((1, p_all), i32),
            pltpu.VMEM((LINES, 1, q_own), i32),
            pltpu.VMEM((1, p_own), f32),
            pltpu.VMEM((1, q_own), f32),
            pltpu.VMEM((p_own, width * q_own), bf16),
            pltpu.VMEM((LINES, width * q_own, q_own), bf16),
            pltpu.VMEM((LINES, width * q_own, q_own), bf16),
            pltpu.VMEM((LINES, width - 1, q_own // CORES, q_own), bf16),
            pltpu.VMEM((width, q_own, q_own), bf16),
            pltpu.VMEM((p_all, q_own), bf16),
            pltpu.VMEM((p_own, p_all), bf16),
            pltpu.VMEM((p_own, q_own), f32),
            pltpu.VMEM((p_own // ROWS, q_own // HALVES), f32),
            pltpu.VMEM((LINES - 1, p_own, q_own), jnp.int16),
            pltpu.VMEM(((LINES - 1) * ROWS, 1, q_own), f32),
            pltpu.VMEM((LINES, p_own, q_own), jnp.int16),
            pltpu.VMEM((LINES * ROWS, 1, q_own), f32),
            pltpu.VMEM((q_own, p_own), f32),
            pltpu.VMEM((width, 1, q_own), i32),
            pltpu.VMEM((width, early, q_own), jnp.int16),
            pltpu.VMEM((width, 1, q_own), f32),
            pltpu.VMEM((width - 1, early, q_own), jnp.int16),
            pltpu.VMEM((width - 1, 1, q_own), f32),
            pltpu.VMEM((width - 1, early, q_own), jnp.int16),
            pltpu.VMEM((width - 1, 1, q_own), f32),
            dma((width - 1, ROWS)),
            dma((width - 1, ROWS)),
            dma((width - 1, LINES, HALVES)),
            dma((width - 1, LINES, HALVES, CORES)),
            dma((width - 1, LINES, HALVES)),
            dma((occ_size - 1,)),
            dma((occ_size,)),
            dma((LINES - 1, HALVES, ROWS)),
            dma((LINES, HALVES, ROWS)),
            dma((LINES - 1, HALVES, ROWS)),
            dma((LINES, HALVES, ROWS)),
            dma((LINES, width - 1)),
            dma((LINES,)),
            dma((7,)),
            dma((HALVES, ROWS)),
            dma((width,)),
            dma((2, width)),
            dma((2, width)),
            dma((2, width - 1)),
            dma((2, width - 1)),
        ],
        compiler_params=pltpu.CompilerParams(
            collective_id=0, has_side_effects=True, vmem_limit_bytes=60 * 1024 * 1024
        ),
    )(
        amplitudes, hole_integrals, particle_integrals, occ_irrep, vir_irrep,
        occ_energy[None, :], vir_energy[None, :],
    )


def solution(mesh):
    placed = (P("occ", "vir"), P("occ", None), P("vir", None), P(), P(), P("occ"), P("vir"))
    return jax.shard_map(
        functools.partial(per_device, mesh.shape["occ"], mesh.shape["vir"]),
        mesh=mesh, in_specs=placed, out_specs=P("vir", "occ"), check_vma=False,
    )
```

```python
import functools

import jax
import jax.numpy as jnp
from jax import lax
from jax.experimental import pallas as pl
from jax.experimental.pallas import tpu as pltpu
from jax.sharding import PartitionSpec as P

TILE = 64
CORES = 2
LANES = 128
QUARTERS = 2 * CORES
LINES = 4
EIGHTHS = (3, 1, 2, 2)
ROWS = len(EIGHTHS)
PAIR_PIECES = 4
HALVES = 2
EARLY = 1
TOP = 32000.0
MESH = pl.DeviceIdType.MESH
ORDER = ("v0", "v1", "t0", "t1", "t2", "v2", "t3", "v3", "v4", "v5", "v6", "v7")
OUTER = (
    "a0", "a1", "p1", "p2", "b0", "c0", "t0", "b1", "c1", "t1", "e0", "t2", "a2", "t3", "a3", "b2",
    "c2", "a4", "q0", "a5", "a6", "b3", "c3", "a7", "p3", "b4", "c4", "q1", "b5", "q2", "c5", "b6",
    "c6", "b7", "c7", "q3", "h0",
)
INNER = (
    "a0", "a1", "p1", "p2", "b0", "c0", "t0", "b1", "c1", "t1", "e0", "t2", "a2", "m00", "m01", "t3",
    "m10", "m11", "a3", "b2", "m20", "c2", "a4", "m21", "q0", "a5", "m30", "a6", "b3", "m31", "c3", "a7",
    "p3", "b4", "c4", "q1", "b5", "m02", "q2", "m12", "c5", "b6", "m22", "c6", "b7", "m32", "c7", "q3",
    "m03", "m13", "m23", "m33", "h0",
)


def kernel(
    width, groups, amp, hole, slab, occ_irrep, vir_irrep, occ_e, vir_e, out,
    occ_tags, vir_tags, occ_labels, vir_labels, occ_row, vir_row,
    t_all, v_all, v_masked, v_send, v_mate, cols_all, hole_all, acc, box_out, scale_out, box_in, scale_in, result,
    mate_labels, early_out, early_scale_out, early_in, early_scale_in, extra_in, extra_scale_in, gauge,
    sent, t_sem, v_sem, pair_sem, box_sem, local_sem, own_sem, load_sem, out_sem, mate_load, early_sem, extra_sem,
):
    p_own, q_own = amp.shape
    o, v = lax.axis_index("occ"), lax.axis_index("vir")
    c = lax.rem(o, CORES)
    z, x = v // width, lax.rem(v, width)
    occ_size = groups * CORES
    partner = o + 1 - 2 * c
    half = z // 2
    mid = lax.rem(z + half, 2)
    mate, far, near = z + 1 - 2 * lax.rem(z, 2), 3 * (1 - half), 2 - half
    owner = [far, near, mate, z]
    target = [mid * far + (1 - mid) * mate, mid * near + (1 - mid) * mate, mate]
    box = [2 - mid, 3 - 2 * mid, 0]
    rows, cols, share = p_own // PAIR_PIECES, q_own // HALVES, q_own // QUARTERS
    starts = [sum(EIGHTHS[:i]) * p_own // 8 for i in range(ROWS + 1)]
    group, odd = o // CORES, lax.rem(o // CORES, 2)
    across = o + CORES - 2 * CORES * odd
    mine, opposite = odd * CORES + c, (1 - odd) * CORES + c
    tiles = q_own // TILE
    others = range(1, width)
    early = pl.ds(0, starts[EARLY])

    def some(i):
        return pl.ds(starts[i], starts[i + 1] - starts[i])


    def xdev(k):
        return (o, z * width + lax.rem(x + k, width))

    def remote(src, dst, send, recv, device):
        return pltpu.make_async_remote_copy(
            src_ref=src, dst_ref=dst, send_sem=send, recv_sem=recv, device_id=device, device_id_type=MESH
        )

    def landed(ref, sem):
        pltpu.make_async_copy(ref, ref, sem).wait()

    def both(height, length, sem):
        landed(gauge.at[pl.ds(0, (2 * height * length + 4 * length) // 512)], sem)

    barrier = pltpu.get_barrier_semaphore()
    peers = [(partner, v)] + [(lax.rem(o + CORES * d, occ_size), v) for d in range(1, groups)]
    peers += [xdev(k) for k in others] + [(o, mate * width + x), (o, near * width + x)]
    for peer in peers:
        pl.semaphore_signal(barrier, inc=1, device_id=peer, device_id_type=MESH)

    loads = {}

    def load(name, src, dst, sem):
        loads[name] = pltpu.make_async_copy(src, dst, sem)
        loads[name].start()

    def columns(zz, xx):
        return pl.ds(pl.multiple_of((zz * width + xx) * q_own, q_own), q_own)

    load("amp", amp, t_all.at[:, pl.ds(0, q_own)], load_sem.at[0])
    load("occ_tags", occ_irrep, occ_tags, load_sem.at[1])
    load("vir_tags", vir_irrep, vir_tags, load_sem.at[2])
    for k in range(width):
        load(("mate", k), slab.at[:, columns(mate, lax.rem(x + k, width))], v_mate.at[k], mate_load.at[k])
    for j in range(LINES):
        for k in others:
            load(
                ("send", j, k),
                slab.at[pl.ds(pl.multiple_of(mine * share, share), share), columns(owner[j], lax.rem(x + k, width))],
                v_send.at[j, k - 1], local_sem.at[j, k - 1],
            )
        load(("own", j), slab.at[:, columns(owner[j], x)], v_all.at[j, pl.ds(0, q_own), :], own_sem.at[j])
    load("occ_row", occ_e, occ_row, load_sem.at[3])
    load("vir_row", vir_e, vir_row, load_sem.at[4])
    load("hole", hole, hole_all, load_sem.at[5])

    pl.semaphore_wait(barrier, len(peers) - 1 + 2 * mid)

    def t_copy(i, k):
        at = some(i)
        return remote(
            t_all.at[at, pl.ds(0, q_own)], t_all.at[at, pl.ds((width - k) * q_own, q_own)],
            sent.at[0], t_sem.at[width - k - 1, i], xdev(k),
        )

    def v_piece(j, h, d, quarter):
        return v_all.at[
            j, pl.ds(pl.multiple_of(d * q_own + quarter * share, share), share), pl.ds(h * cols, cols)
        ]

    def v_copy(j, h, k):
        return remote(
            v_send.at[j, k - 1, :, pl.ds(h * cols, cols)], v_piece(j, h, width - k, mine),
            sent.at[1], v_sem.at[width - k - 1, j, h, mine], xdev(k),
        )

    def relay_copies(j, h, d, first=True, second=True):
        piece, sem = v_piece(j, h, d, mine), v_sem.at[d - 1, j, h, mine]
        other, other_sem = v_piece(j, h, d, opposite), v_sem.at[d - 1, j, h, opposite]
        copies = []
        if first:
            copies.append(remote(piece, piece, sent.at[2], sem, (across, v)))
            copies.append(remote(piece, piece, sent.at[3], sem, (partner, v)))
        if second:
            copies.append(remote(other, other, sent.at[4], other_sem, (partner, v)))
        return copies

    def pair_rows(oo, i):
        return cols_all.at[pl.ds(pl.multiple_of(oo * p_own + i * rows, rows), rows), :]

    def pair_copy(i, d):
        device = partner if d == 0 else lax.rem(o + CORES * d, occ_size)
        return remote(
            t_all.at[pl.ds(i * rows, rows), pl.ds(0, q_own)], pair_rows(o, i), sent.at[5], pair_sem.at[o, i], (device, v)
        )

    def pass_copy(i, d):
        oo = lax.rem(o + CORES * d, occ_size)
        return remote(pair_rows(oo, i), pair_rows(oo, i), sent.at[6], pair_sem.at[oo, i], (partner, v))

    fetched = set()

    def x_send(kind, n):
        for k in others:
            if kind == "t":
                t_copy(n, k).start()
                continue
            j, h = divmod(n, HALVES)
            if (j, k) not in fetched:
                fetched.add((j, k))
                loads["send", j, k].wait()
            v_copy(j, h, k).start()

    loads["amp"].wait()
    for step in ORDER:
        x_send(step[0], int(step[1:]))
        if step == "t0":
            for d in range(1, groups):
                pair_copy(0, d).start()
    for i in range(PAIR_PIECES):
        pair_copy(i, 0).start()
    load("pairs", amp, cols_all.at[pl.ds(pl.multiple_of(o * p_own, p_own), p_own), :], load_sem.at[6])

    loads["occ_tags"].wait()
    loads["vir_tags"].wait()
    low = lax.broadcasted_iota(jnp.int32, (1, 2 * TILE), 1) < TILE

    def label(ref, j, zz, xx):
        base = (zz * width + xx) * tiles

        @pl.loop(0, tiles // 2)
        def _(i):
            at = pl.ds(pl.multiple_of(i * 2 * TILE, 2 * TILE), 2 * TILE)
            ref[j, :, at] = jnp.where(low, vir_tags[base + 2 * i], vir_tags[base + 2 * i + 1])

    def pack(part):
        most = jnp.maximum(jnp.max(jnp.abs(part), axis=0, keepdims=True), 1e-30)
        return jnp.round(part * (TOP / most)).astype(jnp.int32).astype(jnp.int16), most * (1.0 / TOP)

    def early_copies(k):
        land, where = (box_in.at[0, early, :], scale_in.at[0]) if k == 0 else (early_in.at[k - 1], early_scale_in.at[k - 1])
        device = (o, mate * width + x)
        return (
            remote(early_out.at[k], land, sent.at[7], early_sem.at[0, k], device),
            remote(early_scale_out.at[k], where, sent.at[8], early_sem.at[0, k], device),
        )

    def extra_copies(k):
        return (
            remote(early_in.at[k - 1], extra_in.at[width - k - 1], sent.at[9], extra_sem.at[0, width - k - 1], xdev(k)),
            remote(
                early_scale_in.at[k - 1], extra_scale_in.at[width - k - 1],
                sent.at[10], extra_sem.at[0, width - k - 1], xdev(k),
            ),
        )

    for k in reversed(range(width)):
        label(mate_labels, k, mate, lax.rem(x + k, width))
        loads["mate", k].wait()

        @pl.loop(0, tiles)
        def _(i):
            part = pl.ds(pl.multiple_of(i * TILE, TILE), TILE)
            keep = (mate_labels[k] == vir_tags[(z * width + x) * tiles + i]).astype(jnp.float32).astype(jnp.bfloat16)
            v_mate[k, part, :] = v_mate[k, part, :] * keep

        early_out[k], early_scale_out[k] = pack(
            jnp.dot(t_all[early, pl.ds(0, q_own)], v_mate[k], preferred_element_type=jnp.float32)
        )
        for copy in early_copies(k):
            copy.start()

    for j in range(LINES):
        label(vir_labels, j, owner[j], x)

    @pl.loop(0, occ_tags.shape[0] // 2)
    def _(i):
        at = pl.ds(pl.multiple_of(i * 2 * TILE, 2 * TILE), 2 * TILE)
        occ_labels[:, at] = jnp.where(low, occ_tags[2 * i], occ_tags[2 * i + 1])

    def mask(j, d, at):
        first = (z * width + lax.rem(x + d, width)) * tiles
        labels = vir_labels[j, :, at]

        @pl.loop(0, tiles)
        def _(i):
            part = pl.ds(pl.multiple_of(d * q_own + i * TILE, TILE), TILE)
            keep = (labels == vir_tags[first + i]).astype(jnp.float32).astype(jnp.bfloat16)
            v_masked[j, part, at] = v_all[j, part, at] * keep

    everything = pl.ds(0, q_own)
    loads["own", 0].wait()
    mask(0, 0, everything)

    loads["hole"].wait()

    @pl.loop(0, p_own // TILE)
    def _(i):
        at = pl.ds(pl.multiple_of(i * TILE, TILE), TILE)
        keep = (occ_labels[...] == occ_tags[o * (p_own // TILE) + i]).astype(jnp.float32).astype(jnp.bfloat16)
        hole_all[at, :] = hole_all[at, :] * keep

    def box_copies(j, h, i):
        at, there = some(i), pl.ds(h * cols, cols)
        device = (o, target[j] * width + x)
        return (
            remote(
                box_out.at[j, at, there], box_in.at[box[j], at, there],
                sent.at[11 + j // 2], box_sem.at[box[j], h, i], device,
            ),
            remote(
                scale_out.at[j * ROWS + i, :, there], scale_in.at[box[j] * ROWS + i, :, there],
                sent.at[13 + j // 2], box_sem.at[box[j], h, i], device,
            ),
        )

    def arrived(b, h, i):
        at, there = some(i), pl.ds(h * cols, cols)
        both(starts[i + 1] - starts[i], cols, box_sem.at[b, h, i])
        return box_in[b, at, there].astype(jnp.float32) * scale_in[b * ROWS + i, :, there]

    def unit(j, h, i, merge=False):
        at, there = some(i), pl.ds(h * cols, cols)
        part = jnp.dot(t_all[at, :], v_masked[j, :, there], preferred_element_type=jnp.float32)
        if j == LINES - 1:
            acc[at, there] = part
            return
        if merge:
            part = part + arrived(j + 2, h, i)
        box_out[j, at, there], scale_out[j * ROWS + i, :, there] = pack(part)
        for copy in box_copies(j, h, i):
            copy.start()

    def skipped(j, i, inner):
        return (inner and j < LINES - 2) or (j == LINES - 2 and i < EARLY)

    def act(kind, n, i, inner, have_t, have_v):
        j, h = divmod(n, HALVES)
        if kind == "t":
            for d in others:
                landed(t_all.at[some(n), pl.ds(d * q_own, q_own)], t_sem.at[d - 1, n])
            have_t.append(n)
            for jj, hh in have_v:
                if not skipped(jj, n, inner):
                    unit(jj, hh, n)
        elif kind == "a":
            for d in others:
                landed(v_piece(j, h, d, mine), v_sem.at[d - 1, j, h, mine])
                for copy in relay_copies(j, h, d, second=False):
                    copy.start()
        elif kind == "b":
            for d in others:
                landed(v_piece(j, h, d, opposite), v_sem.at[d - 1, j, h, opposite])
                relay_copies(j, h, d, first=False)[0].start()
            if h == 0 and j > 0:
                loads["own", j].wait()
                mask(j, 0, everything)
        elif kind == "c":
            for d in others:
                for odds in (odd, 1 - odd):
                    quarter = odds * CORES + 1 - c
                    landed(v_piece(j, h, d, quarter), v_sem.at[d - 1, j, h, quarter])
                mask(j, d, pl.ds(h * cols, cols))
            have_v.append((j, h))
            for t in have_t:
                if not skipped(j, t, inner):
                    unit(j, h, t)
        elif kind == "m":
            unit(j, h, i, merge=True)
        elif kind == "p":
            for d in range(1, groups):
                pair_copy(n, d).start()
        elif kind == "q":
            for d in range(1, groups):
                oo = lax.rem(o + CORES * d, occ_size)
                landed(pair_rows(oo, n), pair_sem.at[oo, n])
                pass_copy(n, d).start()
        elif kind == "e":
            for k in others:
                both(starts[EARLY], q_own, early_sem.at[0, k])
                for copy in extra_copies(k):
                    copy.start()
        else:
            loads["pairs"].wait()
            for d in range(groups):
                oo = lax.rem(partner + CORES * d, occ_size)
                for i in range(PAIR_PIECES):
                    landed(pair_rows(oo, i), pair_sem.at[oo, i])

            @pl.loop(0, PAIR_PIECES)
            def _(i):
                at = pl.ds(pl.multiple_of(i * rows, rows), rows)
                acc[at, :] += jnp.dot(hole_all[at, :], cols_all[...], preferred_element_type=jnp.float32)

    def run(actions, inner):
        have_t, have_v = [], []
        for action in actions:
            act(action[0], int(action[-1]), int(action[1]), inner, have_t, have_v)

    pl.when(mid == 0)(lambda: run(OUTER, False))
    pl.when(mid == 1)(lambda: run(INNER, True))
    loads["occ_row"].wait()
    loads["vir_row"].wait()
    for i in range(PAIR_PIECES):
        at = pl.ds(i * rows, rows)
        result[:, at] = 1.0 / (jnp.broadcast_to(vir_row[...], (rows, q_own)).T - occ_row[:, at])

    for h in range(HALVES):
        for i in range(ROWS):
            acc[some(i), pl.ds(h * cols, cols)] += arrived(1, h, i)

    both(starts[EARLY], q_own, early_sem.at[0, 0])
    acc[early, :] += box_in[0, early, :].astype(jnp.float32) * scale_in[0]
    for d in others:
        both(starts[EARLY], q_own, extra_sem.at[0, d - 1])
        acc[early, :] += extra_in[d - 1].astype(jnp.float32) * extra_scale_in[d - 1]

    ends = [0] + [i + 1 for i in range(ROWS) if starts[i + 1] % LANES == 0]
    spans = list(zip(ends[:-1], ends[1:]))

    def span(first, last):
        return pl.ds(starts[first], starts[last] - starts[first])

    def out_copy(h, first, last):
        at, there = span(first, last), pl.ds(h * cols, cols)
        return pltpu.make_async_copy(result.at[there, at], out.at[there, at], out_sem.at[0])

    for h in range(HALVES):
        there = pl.ds(h * cols, cols)
        if h == HALVES - 1:
            for n, ref in enumerate((
                t_all.at[:, pl.ds(0, (width - 1) * q_own)], v_send, v_send, v_send, v_send,
                cols_all.at[pl.ds(0, groups * p_own), :], cols_all.at[pl.ds(0, (groups - 1) * p_own), :],
                early_out, early_scale_out, early_in, early_scale_in,
                box_out.at[pl.ds(0, LINES - 2)], box_out.at[LINES - 2, pl.ds(starts[EARLY], p_own - starts[EARLY]), :],
                scale_out.at[pl.ds(0, (LINES - 2) * ROWS)],
                scale_out.at[pl.ds((LINES - 2) * ROWS + EARLY, ROWS - EARLY)],
            )):
                landed(ref, sent.at[n])

        for first, last in spans:
            for i in range(max(first, EARLY), last):
                acc[some(i), there] += arrived(0, h, i)
            at = span(first, last)
            result[there, at] = acc[at, there].T * result[there, at]
            out_copy(h, first, last).start()

    landed(result, out_sem.at[0])


def per_device(
    occ_size, vir_size, amplitudes, hole_integrals, particle_integrals, occ_irrep, vir_irrep, occ_energy, vir_energy
):
    width, groups = vir_size // LINES, occ_size // CORES
    p_own, q_own = amplitudes.shape
    p_all, early = p_own * occ_size, sum(EIGHTHS[:EARLY]) * p_own // 8
    bf16, f32, i32 = jnp.bfloat16, jnp.float32, jnp.int32
    dma = pltpu.SemaphoreType.DMA
    anywhere = pl.BlockSpec(memory_space=pl.ANY)
    return pl.pallas_call(
        functools.partial(kernel, width, groups),
        out_shape=jax.ShapeDtypeStruct((q_own, p_own), f32),
        in_specs=[anywhere] * 7,
        out_specs=anywhere,
        scratch_shapes=[
            pltpu.SMEM(occ_irrep.shape, i32),
            pltpu.SMEM(vir_irrep.shape, i32),
            pltpu.VMEM((1, p_all), i32),
            pltpu.VMEM((LINES, 1, q_own), i32),
            pltpu.VMEM((1, p_own), f32),
            pltpu.VMEM((1, q_own), f32),
            pltpu.VMEM((p_own, width * q_own), bf16),
            pltpu.VMEM((LINES, width * q_own, q_own), bf16),
            pltpu.VMEM((LINES, width * q_own, q_own), bf16),
            pltpu.VMEM((LINES, width - 1, q_own // QUARTERS, q_own), bf16),
            pltpu.VMEM((width, q_own, q_own), bf16),
            pltpu.VMEM((p_all, q_own), bf16),
            pltpu.VMEM((p_own, p_all), bf16),
            pltpu.VMEM((p_own, q_own), f32),
            pltpu.VMEM((LINES - 1, p_own, q_own), jnp.int16),
            pltpu.VMEM(((LINES - 1) * ROWS, 1, q_own), f32),
            pltpu.VMEM((LINES, p_own, q_own), jnp.int16),
            pltpu.VMEM((LINES * ROWS, 1, q_own), f32),
            pltpu.VMEM((q_own, p_own), f32),
            pltpu.VMEM((width, 1, q_own), i32),
            pltpu.VMEM((width, early, q_own), jnp.int16),
            pltpu.VMEM((width, 1, q_own), f32),
            pltpu.VMEM((width - 1, early, q_own), jnp.int16),
            pltpu.VMEM((width - 1, 1, q_own), f32),
            pltpu.VMEM((width - 1, early, q_own), jnp.int16),
            pltpu.VMEM((width - 1, 1, q_own), f32),
            pltpu.VMEM(((2 * p_own * q_own + 4 * q_own) // 512, 1, LANES), f32),
            dma((15,)),
            dma((width - 1, ROWS)),
            dma((width - 1, LINES, HALVES, QUARTERS)),
            dma((occ_size, PAIR_PIECES)),
            dma((LINES, HALVES, ROWS)),
            dma((LINES, width - 1)),
            dma((LINES,)),
            dma((7,)),
            dma((1,)),
            dma((width,)),
            dma((1, width)),
            dma((1, width - 1)),
        ],
        compiler_params=pltpu.CompilerParams(
            collective_id=0, has_side_effects=True, vmem_limit_bytes=60 * 1024 * 1024
        ),
    )(
        amplitudes, hole_integrals, particle_integrals, occ_irrep, vir_irrep,
        occ_energy[None, :], vir_energy[None, :],
    )


def solution(mesh):
    placed = (P("occ", "vir"), P("occ", None), P("vir", None), P(), P(), P("occ"), P("vir"))
    return jax.shard_map(
        functools.partial(per_device, mesh.shape["occ"], mesh.shape["vir"]),
        mesh=mesh, in_specs=placed, out_specs=P("vir", "occ"), check_vma=False,
    )
```

```python
import functools

import jax
import jax.numpy as jnp
from jax import lax
from jax.experimental import pallas as pl
from jax.experimental.pallas import tpu as pltpu
from jax.sharding import PartitionSpec as P

TILE = 64
CORES = 2
LANES = 128
QUARTERS = 2 * CORES
LINES = 4
EIGHTHS = (3, 1, 2, 2)
ROWS = len(EIGHTHS)
PAIR_PIECES = 4
HALVES = 2
EARLY = 1
TOP = 32000.0
MESH = pl.DeviceIdType.MESH
ORDER = ("v0", "v1", "t0", "t1", "t2", "v2", "t3", "v3", "v4", "v5", "v6", "v7")
OUTER = (
    "a0", "a1", "b0", "g0", "c0", "p1", "t0", "b1", "c1", "t1", "e0", "t2", "p2", "a2", "t3", "a3",
    "b2", "r0", "c2", "a4", "q0", "a5", "a6", "b3", "c3", "a7", "p3", "b4", "c4", "q1", "q2", "b5",
    "c5", "b6", "c6", "b7", "c7", "q3", "h0",
)
INNER = (
    "a0", "a1", "b0", "g0", "c0", "p1", "t0", "b1", "m00", "c1", "t1", "m01", "m10", "e0", "m11", "t2",
    "p2", "m20", "a2", "m21", "t3", "m30", "m31", "a3", "b2", "r0", "c2", "a4", "m02", "q0", "m12", "a5",
    "m22", "a6", "b3", "m32", "c3", "a7", "p3", "b4", "c4", "q1", "q2", "b5", "m03", "m13", "c5", "b6",
    "m23", "c6", "b7", "m33", "c7", "q3", "h0",
)


def kernel(
    width, groups, amp, hole, slab, occ_irrep, vir_irrep, occ_e, vir_e, out,
    occ_tags, vir_tags, occ_labels, vir_labels, occ_row, vir_row,
    t_all, v_all, v_masked, v_send, v_mate, cols_all, hole_all, acc, box_out, scale_out, box_in, scale_in, result,
    mate_labels, early_out, early_scale_out, early_in, early_scale_in, extra_in, extra_scale_in, gauge,
    sent, t_sem, v_sem, pair_sem, box_sem, local_sem, own_sem, load_sem, out_sem, mate_load, early_sem, extra_sem,
):
    p_own, q_own = amp.shape
    o, v = lax.axis_index("occ"), lax.axis_index("vir")
    c = lax.rem(o, CORES)
    z, x = v // width, lax.rem(v, width)
    occ_size = groups * CORES
    partner = o + 1 - 2 * c
    half = z // 2
    mid = lax.rem(z + half, 2)
    mate, far, near = z + 1 - 2 * lax.rem(z, 2), 3 * (1 - half), 2 - half
    owner = [far, near, mate, z]
    target = [mid * far + (1 - mid) * mate, mid * near + (1 - mid) * mate, mate]
    box = [2 - mid, 3 - 2 * mid, 0]
    rows, cols, share = p_own // PAIR_PIECES, q_own // HALVES, q_own // QUARTERS
    starts = [sum(EIGHTHS[:i]) * p_own // 8 for i in range(ROWS + 1)]
    group, odd = o // CORES, lax.rem(o // CORES, 2)
    across = o + CORES - 2 * CORES * odd
    mine, opposite = odd * CORES + c, (1 - odd) * CORES + c
    tiles = q_own // TILE
    others = range(1, width)
    early = pl.ds(0, starts[EARLY])

    def some(i):
        return pl.ds(starts[i], starts[i + 1] - starts[i])


    def xdev(k):
        return (o, z * width + lax.rem(x + k, width))

    def remote(src, dst, send, recv, device):
        return pltpu.make_async_remote_copy(
            src_ref=src, dst_ref=dst, send_sem=send, recv_sem=recv, device_id=device, device_id_type=MESH
        )

    def landed(ref, sem):
        pltpu.make_async_copy(ref, ref, sem).wait()

    def both(height, length, sem):
        landed(gauge.at[pl.ds(0, (2 * height * length + 4 * length) // 512)], sem)

    barrier = pltpu.get_barrier_semaphore()
    peers = [(partner, v)] + [(lax.rem(o + CORES * d, occ_size), v) for d in range(1, groups)]
    peers += [xdev(k) for k in others] + [(o, mate * width + x), (o, near * width + x)]
    for peer in peers:
        pl.semaphore_signal(barrier, inc=1, device_id=peer, device_id_type=MESH)

    loads = {}

    def load(name, src, dst, sem):
        loads[name] = pltpu.make_async_copy(src, dst, sem)
        loads[name].start()

    def columns(zz, xx):
        return pl.ds(pl.multiple_of((zz * width + xx) * q_own, q_own), q_own)

    load("amp", amp, t_all.at[:, pl.ds(0, q_own)], load_sem.at[0])
    load("occ_tags", occ_irrep, occ_tags, load_sem.at[1])
    load("vir_tags", vir_irrep, vir_tags, load_sem.at[2])
    for k in range(width):
        load(("mate", k), slab.at[:, columns(mate, lax.rem(x + k, width))], v_mate.at[k], mate_load.at[k])
    for j in range(LINES):
        for k in others:
            load(
                ("send", j, k),
                slab.at[pl.ds(pl.multiple_of(mine * share, share), share), columns(owner[j], lax.rem(x + k, width))],
                v_send.at[j, k - 1], local_sem.at[j, k - 1],
            )
        load(("own", j), slab.at[:, columns(owner[j], x)], v_all.at[j, pl.ds(0, q_own), :], own_sem.at[j])
    load("occ_row", occ_e, occ_row, load_sem.at[3])
    load("vir_row", vir_e, vir_row, load_sem.at[4])
    load("hole", hole, hole_all, load_sem.at[5])

    pl.semaphore_wait(barrier, len(peers) - 1 + 2 * mid)

    def t_copy(i, k):
        at = some(i)
        return remote(
            t_all.at[at, pl.ds(0, q_own)], t_all.at[at, pl.ds((width - k) * q_own, q_own)],
            sent.at[0], t_sem.at[width - k - 1, i], xdev(k),
        )

    def v_piece(j, h, d, quarter):
        return v_all.at[
            j, pl.ds(pl.multiple_of(d * q_own + quarter * share, share), share), pl.ds(h * cols, cols)
        ]

    def v_copy(j, h, k):
        return remote(
            v_send.at[j, k - 1, :, pl.ds(h * cols, cols)], v_piece(j, h, width - k, mine),
            sent.at[1], v_sem.at[width - k - 1, j, h, mine], xdev(k),
        )

    def relay_copies(j, h, d, first=True, second=True):
        piece, sem = v_piece(j, h, d, mine), v_sem.at[d - 1, j, h, mine]
        other, other_sem = v_piece(j, h, d, opposite), v_sem.at[d - 1, j, h, opposite]
        copies = []
        if first:
            copies.append(remote(piece, piece, sent.at[2], sem, (across, v)))
            copies.append(remote(piece, piece, sent.at[3], sem, (partner, v)))
        if second:
            copies.append(remote(other, other, sent.at[4], other_sem, (partner, v)))
        return copies

    def pair_rows(oo, i):
        return cols_all.at[pl.ds(pl.multiple_of(oo * p_own + i * rows, rows), rows), :]

    def pair_copy(i, d):
        device = partner if d == 0 else lax.rem(o + CORES * d, occ_size)
        return remote(
            t_all.at[pl.ds(i * rows, rows), pl.ds(0, q_own)], pair_rows(o, i), sent.at[5], pair_sem.at[o, i], (device, v)
        )

    def pass_copy(i, d):
        oo = lax.rem(o + CORES * d, occ_size)
        return remote(pair_rows(oo, i), pair_rows(oo, i), sent.at[6], pair_sem.at[oo, i], (partner, v))

    fetched = set()

    def x_send(kind, n):
        for k in others:
            if kind == "t":
                t_copy(n, k).start()
                continue
            j, h = divmod(n, HALVES)
            if (j, k) not in fetched:
                fetched.add((j, k))
                loads["send", j, k].wait()
            v_copy(j, h, k).start()

    loads["amp"].wait()
    for step in ORDER:
        x_send(step[0], int(step[1:]))
        if step == "t0":
            for d in range(1, groups):
                pair_copy(0, d).start()
    for i in range(PAIR_PIECES):
        pair_copy(i, 0).start()
    load("pairs", amp, cols_all.at[pl.ds(pl.multiple_of(o * p_own, p_own), p_own), :], load_sem.at[6])

    loads["occ_tags"].wait()
    loads["vir_tags"].wait()
    low = lax.broadcasted_iota(jnp.int32, (1, 2 * TILE), 1) < TILE

    def label(ref, j, zz, xx):
        base = (zz * width + xx) * tiles

        @pl.loop(0, tiles // 2)
        def _(i):
            at = pl.ds(pl.multiple_of(i * 2 * TILE, 2 * TILE), 2 * TILE)
            ref[j, :, at] = jnp.where(low, vir_tags[base + 2 * i], vir_tags[base + 2 * i + 1])

    def pack(part):
        most = jnp.maximum(jnp.max(jnp.abs(part), axis=0, keepdims=True), 1e-30)
        return jnp.round(part * (TOP / most)).astype(jnp.int32).astype(jnp.int16), most * (1.0 / TOP)

    def early_copies(k):
        land, where = (box_in.at[0, early, :], scale_in.at[0]) if k == 0 else (early_in.at[k - 1], early_scale_in.at[k - 1])
        device = (o, mate * width + x)
        return (
            remote(early_out.at[k], land, sent.at[7], early_sem.at[0, k], device),
            remote(early_scale_out.at[k], where, sent.at[8], early_sem.at[0, k], device),
        )

    def extra_copies(k):
        return (
            remote(early_in.at[k - 1], extra_in.at[width - k - 1], sent.at[9], extra_sem.at[0, width - k - 1], xdev(k)),
            remote(
                early_scale_in.at[k - 1], extra_scale_in.at[width - k - 1],
                sent.at[10], extra_sem.at[0, width - k - 1], xdev(k),
            ),
        )

    for k in reversed(range(width)):
        label(mate_labels, k, mate, lax.rem(x + k, width))
        loads["mate", k].wait()

        @pl.loop(0, tiles)
        def _(i):
            part = pl.ds(pl.multiple_of(i * TILE, TILE), TILE)
            keep = (mate_labels[k] == vir_tags[(z * width + x) * tiles + i]).astype(jnp.float32).astype(jnp.bfloat16)
            v_mate[k, part, :] = v_mate[k, part, :] * keep

        early_out[k], early_scale_out[k] = pack(
            jnp.dot(t_all[early, pl.ds(0, q_own)], v_mate[k], preferred_element_type=jnp.float32)
        )
        for copy in early_copies(k):
            copy.start()

    for j in range(LINES):
        label(vir_labels, j, owner[j], x)

    @pl.loop(0, occ_tags.shape[0] // 2)
    def _(i):
        at = pl.ds(pl.multiple_of(i * 2 * TILE, 2 * TILE), 2 * TILE)
        occ_labels[:, at] = jnp.where(low, occ_tags[2 * i], occ_tags[2 * i + 1])

    def mask(j, d, at):
        first = (z * width + lax.rem(x + d, width)) * tiles
        labels = vir_labels[j, :, at]

        @pl.loop(0, tiles)
        def _(i):
            part = pl.ds(pl.multiple_of(d * q_own + i * TILE, TILE), TILE)
            keep = (labels == vir_tags[first + i]).astype(jnp.float32).astype(jnp.bfloat16)
            v_masked[j, part, at] = v_all[j, part, at] * keep

    everything = pl.ds(0, q_own)
    loads["own", 0].wait()
    mask(0, 0, everything)

    loads["hole"].wait()

    @pl.loop(0, p_own // TILE)
    def _(i):
        at = pl.ds(pl.multiple_of(i * TILE, TILE), TILE)
        keep = (occ_labels[...] == occ_tags[o * (p_own // TILE) + i]).astype(jnp.float32).astype(jnp.bfloat16)
        hole_all[at, :] = hole_all[at, :] * keep

    def box_copies(j, h, i):
        at, there = some(i), pl.ds(h * cols, cols)
        device = (o, target[j] * width + x)
        return (
            remote(
                box_out.at[j, at, there], box_in.at[box[j], at, there],
                sent.at[11 + j // 2], box_sem.at[box[j], h, i], device,
            ),
            remote(
                scale_out.at[j * ROWS + i, :, there], scale_in.at[box[j] * ROWS + i, :, there],
                sent.at[13 + j // 2], box_sem.at[box[j], h, i], device,
            ),
        )

    def arrived(b, h, i):
        at, there = some(i), pl.ds(h * cols, cols)
        both(starts[i + 1] - starts[i], cols, box_sem.at[b, h, i])
        return box_in[b, at, there].astype(jnp.float32) * scale_in[b * ROWS + i, :, there]

    def unit(j, h, i, merge=False):
        at, there = some(i), pl.ds(h * cols, cols)
        part = jnp.dot(t_all[at, :], v_masked[j, :, there], preferred_element_type=jnp.float32)
        if j == LINES - 1:
            acc[at, there] += part
            return
        if merge:
            part = part + arrived(j + 2, h, i)
        box_out[j, at, there], scale_out[j * ROWS + i, :, there] = pack(part)
        for copy in box_copies(j, h, i):
            copy.start()

    def skipped(j, i, inner):
        return (inner and j < LINES - 2) or (j == LINES - 2 and i < EARLY)

    def act(kind, n, i, inner, have_t, have_v):
        j, h = divmod(n, HALVES)
        if kind == "t":
            for d in others:
                landed(t_all.at[some(n), pl.ds(d * q_own, q_own)], t_sem.at[d - 1, n])
            have_t.append(n)
            for jj, hh in have_v:
                if not skipped(jj, n, inner):
                    unit(jj, hh, n)
        elif kind == "a":
            for d in others:
                landed(v_piece(j, h, d, mine), v_sem.at[d - 1, j, h, mine])
                for copy in relay_copies(j, h, d, second=False):
                    copy.start()
        elif kind == "b":
            for d in others:
                landed(v_piece(j, h, d, opposite), v_sem.at[d - 1, j, h, opposite])
                relay_copies(j, h, d, first=False)[0].start()
            if h == 0 and j > 0:
                loads["own", j].wait()
                mask(j, 0, everything)
        elif kind == "c":
            for d in others:
                for odds in (odd, 1 - odd):
                    quarter = odds * CORES + 1 - c
                    landed(v_piece(j, h, d, quarter), v_sem.at[d - 1, j, h, quarter])
                mask(j, d, pl.ds(h * cols, cols))
            have_v.append((j, h))
            for t in have_t:
                if not skipped(j, t, inner):
                    unit(j, h, t)
        elif kind == "m":
            unit(j, h, i, merge=True)
        elif kind == "p":
            for d in range(1, groups):
                pair_copy(n, d).start()
        elif kind == "q":
            for d in range(1, groups):
                oo = lax.rem(o + CORES * d, occ_size)
                landed(pair_rows(oo, n), pair_sem.at[oo, n])
                pass_copy(n, d).start()
        elif kind == "e":
            for k in others:
                both(starts[EARLY], q_own, early_sem.at[0, k])
                for copy in extra_copies(k):
                    copy.start()
        elif kind == "g":
            loads["pairs"].wait()
            for i in range(PAIR_PIECES):
                landed(pair_rows(partner, i), pair_sem.at[partner, i])
            pairs_product(group, False)
        elif kind == "h":
            for d in range(1, groups):
                oo = lax.rem(partner + CORES * d, occ_size)
                for i in range(PAIR_PIECES):
                    landed(pair_rows(oo, i), pair_sem.at[oo, i])
                pairs_product(lax.rem(group + d, groups), True)
        else:
            loads["occ_row"].wait()
            loads["vir_row"].wait()
            for i in range(PAIR_PIECES):
                at = pl.ds(i * rows, rows)
                result[:, at] = 1.0 / (jnp.broadcast_to(vir_row[...], (rows, q_own)).T - occ_row[:, at])

    def pairs_product(g, more):
        both_cores = pl.ds(pl.multiple_of(g * CORES * p_own, CORES * p_own), CORES * p_own)

        @pl.loop(0, PAIR_PIECES)
        def _(i):
            at = pl.ds(pl.multiple_of(i * rows, rows), rows)
            part = jnp.dot(hole_all[at, both_cores], cols_all[both_cores, :], preferred_element_type=jnp.float32)
            acc[at, :] = acc[at, :] + part if more else part

    def run(actions, inner):
        have_t, have_v = [], []
        for action in actions:
            act(action[0], int(action[-1]), int(action[1]), inner, have_t, have_v)

    pl.when(mid == 0)(lambda: run(OUTER, False))
    pl.when(mid == 1)(lambda: run(INNER, True))
    for h in range(HALVES):
        for i in range(ROWS):
            acc[some(i), pl.ds(h * cols, cols)] += arrived(1, h, i)

    both(starts[EARLY], q_own, early_sem.at[0, 0])
    acc[early, :] += box_in[0, early, :].astype(jnp.float32) * scale_in[0]
    for d in others:
        both(starts[EARLY], q_own, extra_sem.at[0, d - 1])
        acc[early, :] += extra_in[d - 1].astype(jnp.float32) * extra_scale_in[d - 1]

    ends = [0] + [i + 1 for i in range(ROWS) if starts[i + 1] % LANES == 0]
    spans = list(zip(ends[:-1], ends[1:]))

    def span(first, last):
        return pl.ds(starts[first], starts[last] - starts[first])

    def out_copy(h, first, last):
        at, there = span(first, last), pl.ds(h * cols, cols)
        return pltpu.make_async_copy(result.at[there, at], out.at[there, at], out_sem.at[0])

    for h in range(HALVES):
        there = pl.ds(h * cols, cols)
        if h == HALVES - 1:
            for n, ref in enumerate((
                t_all.at[:, pl.ds(0, (width - 1) * q_own)], v_send, v_send, v_send, v_send,
                cols_all.at[pl.ds(0, groups * p_own), :], cols_all.at[pl.ds(0, (groups - 1) * p_own), :],
                early_out, early_scale_out, early_in, early_scale_in,
                box_out.at[pl.ds(0, LINES - 2)], box_out.at[LINES - 2, pl.ds(starts[EARLY], p_own - starts[EARLY]), :],
                scale_out.at[pl.ds(0, (LINES - 2) * ROWS)],
                scale_out.at[pl.ds((LINES - 2) * ROWS + EARLY, ROWS - EARLY)],
            )):
                landed(ref, sent.at[n])

        for first, last in spans:
            for i in range(max(first, EARLY), last):
                acc[some(i), there] += arrived(0, h, i)
            at = span(first, last)
            result[there, at] = acc[at, there].T * result[there, at]
            out_copy(h, first, last).start()

    landed(result, out_sem.at[0])


def per_device(
    occ_size, vir_size, amplitudes, hole_integrals, particle_integrals, occ_irrep, vir_irrep, occ_energy, vir_energy
):
    width, groups = vir_size // LINES, occ_size // CORES
    p_own, q_own = amplitudes.shape
    p_all, early = p_own * occ_size, sum(EIGHTHS[:EARLY]) * p_own // 8
    bf16, f32, i32 = jnp.bfloat16, jnp.float32, jnp.int32
    dma = pltpu.SemaphoreType.DMA
    anywhere = pl.BlockSpec(memory_space=pl.ANY)
    return pl.pallas_call(
        functools.partial(kernel, width, groups),
        out_shape=jax.ShapeDtypeStruct((q_own, p_own), f32),
        in_specs=[anywhere] * 7,
        out_specs=anywhere,
        scratch_shapes=[
            pltpu.SMEM(occ_irrep.shape, i32),
            pltpu.SMEM(vir_irrep.shape, i32),
            pltpu.VMEM((1, p_all), i32),
            pltpu.VMEM((LINES, 1, q_own), i32),
            pltpu.VMEM((1, p_own), f32),
            pltpu.VMEM((1, q_own), f32),
            pltpu.VMEM((p_own, width * q_own), bf16),
            pltpu.VMEM((LINES, width * q_own, q_own), bf16),
            pltpu.VMEM((LINES, width * q_own, q_own), bf16),
            pltpu.VMEM((LINES, width - 1, q_own // QUARTERS, q_own), bf16),
            pltpu.VMEM((width, q_own, q_own), bf16),
            pltpu.VMEM((p_all, q_own), bf16),
            pltpu.VMEM((p_own, p_all), bf16),
            pltpu.VMEM((p_own, q_own), f32),
            pltpu.VMEM((LINES - 1, p_own, q_own), jnp.int16),
            pltpu.VMEM(((LINES - 1) * ROWS, 1, q_own), f32),
            pltpu.VMEM((LINES, p_own, q_own), jnp.int16),
            pltpu.VMEM((LINES * ROWS, 1, q_own), f32),
            pltpu.VMEM((q_own, p_own), f32),
            pltpu.VMEM((width, 1, q_own), i32),
            pltpu.VMEM((width, early, q_own), jnp.int16),
            pltpu.VMEM((width, 1, q_own), f32),
            pltpu.VMEM((width - 1, early, q_own), jnp.int16),
            pltpu.VMEM((width - 1, 1, q_own), f32),
            pltpu.VMEM((width - 1, early, q_own), jnp.int16),
            pltpu.VMEM((width - 1, 1, q_own), f32),
            pltpu.VMEM(((2 * p_own * q_own + 4 * q_own) // 512, 1, LANES), f32),
            dma((15,)),
            dma((width - 1, ROWS)),
            dma((width - 1, LINES, HALVES, QUARTERS)),
            dma((occ_size, PAIR_PIECES)),
            dma((LINES, HALVES, ROWS)),
            dma((LINES, width - 1)),
            dma((LINES,)),
            dma((7,)),
            dma((1,)),
            dma((width,)),
            dma((1, width)),
            dma((1, width - 1)),
        ],
        compiler_params=pltpu.CompilerParams(
            collective_id=0, has_side_effects=True, vmem_limit_bytes=60 * 1024 * 1024
        ),
    )(
        amplitudes, hole_integrals, particle_integrals, occ_irrep, vir_irrep,
        occ_energy[None, :], vir_energy[None, :],
    )


def solution(mesh):
    placed = (P("occ", "vir"), P("occ", None), P("vir", None), P(), P(), P("occ"), P("vir"))
    return jax.shard_map(
        functools.partial(per_device, mesh.shape["occ"], mesh.shape["vir"]),
        mesh=mesh, in_specs=placed, out_specs=P("vir", "occ"), check_vma=False,
    )
```

```python
import functools

import jax
import jax.numpy as jnp
from jax import lax
from jax.experimental import pallas as pl
from jax.experimental.pallas import tpu as pltpu
from jax.sharding import PartitionSpec as P

TILE = 64
CORES = 2
LANES = 128
QUARTERS = 2 * CORES
LINES = 4
EIGHTHS = (3, 1, 2, 2)
ROWS = len(EIGHTHS)
PAIR_PIECES = 4
HALVES = 2
EARLY = 1
TOP = 32000.0
MESH = pl.DeviceIdType.MESH
ORDER = ("v0", "v1", "t0", "t1", "t2", "v2", "t3", "v3", "v4", "v5", "v6", "v7")
OUTER = (
    "a0", "a1", "b0", "g0", "c0", "p1", "t0", "b1", "c1", "t1", "e0", "t2", "p2", "a2", "t3", "a3",
    "b2", "r0", "c2", "a4", "q0", "a5", "a6", "b3", "c3", "a7", "p3", "b4", "c4", "q1", "q2", "b5",
    "c5", "b6", "c6", "b7", "c7", "q3", "h0",
)
INNER = (
    "a0", "a1", "b0", "g0", "c0", "p1", "t0", "b1", "m00", "c1", "t1", "m01", "m10", "e0", "m11", "t2",
    "p2", "m20", "a2", "m21", "t3", "m30", "m31", "a3", "b2", "r0", "c2", "a4", "m02", "q0", "m12", "a5",
    "m22", "a6", "b3", "m32", "c3", "a7", "p3", "b4", "c4", "q1", "q2", "b5", "m03", "m13", "c5", "b6",
    "m23", "c6", "b7", "m33", "c7", "q3", "h0",
)


def kernel(
    width, groups, amp, hole, slab, occ_irrep, vir_irrep, occ_e, vir_e, out,
    occ_tags, vir_tags, occ_labels, vir_labels, occ_row, vir_row,
    t_all, v_all, v_masked, v_send, v_mate, cols_all, hole_all, acc, box_out, scale_out, box_in, scale_in, result,
    mate_labels, early_out, early_scale_out, early_in, early_scale_in, extra_in, extra_scale_in, gauge,
    sent, t_sem, v_sem, pair_sem, pass_sem, box_sem, local_sem, own_sem, load_sem, out_sem, mate_load, early_sem, extra_sem,
):
    p_own, q_own = amp.shape
    o, v = lax.axis_index("occ"), lax.axis_index("vir")
    c = lax.rem(o, CORES)
    z, x = v // width, lax.rem(v, width)
    occ_size = groups * CORES
    partner = o + 1 - 2 * c
    half = z // 2
    mid = lax.rem(z + half, 2)
    mate, far, near = z + 1 - 2 * lax.rem(z, 2), 3 * (1 - half), 2 - half
    owner = [far, near, mate, z]
    target = [mid * far + (1 - mid) * mate, mid * near + (1 - mid) * mate, mate]
    box = [2 - mid, 3 - 2 * mid, 0]
    rows, cols, share = p_own // PAIR_PIECES, q_own // HALVES, q_own // QUARTERS
    starts = [sum(EIGHTHS[:i]) * p_own // 8 for i in range(ROWS + 1)]
    group, odd = o // CORES, lax.rem(o // CORES, 2)
    across = o + CORES - 2 * CORES * odd
    mine, opposite = odd * CORES + c, (1 - odd) * CORES + c
    tiles = q_own // TILE
    others = range(1, width)
    early = pl.ds(0, starts[EARLY])

    def some(i):
        return pl.ds(starts[i], starts[i + 1] - starts[i])


    def xdev(k):
        return (o, z * width + lax.rem(x + k, width))

    def remote(src, dst, send, recv, device):
        return pltpu.make_async_remote_copy(
            src_ref=src, dst_ref=dst, send_sem=send, recv_sem=recv, device_id=device, device_id_type=MESH
        )

    def landed(ref, sem):
        pltpu.make_async_copy(ref, ref, sem).wait()

    def both(height, length, sem):
        landed(gauge.at[pl.ds(0, (2 * height * length + 4 * length) // 512)], sem)

    barrier = pltpu.get_barrier_semaphore()
    peers = [(partner, v)] + [(lax.rem(o + CORES * d, occ_size), v) for d in range(1, groups)]
    peers += [xdev(k) for k in others] + [(o, mate * width + x), (o, near * width + x)]
    for peer in peers:
        pl.semaphore_signal(barrier, inc=1, device_id=peer, device_id_type=MESH)

    loads = {}

    def load(name, src, dst, sem):
        loads[name] = pltpu.make_async_copy(src, dst, sem)
        loads[name].start()

    def columns(zz, xx):
        return pl.ds(pl.multiple_of((zz * width + xx) * q_own, q_own), q_own)

    load("amp", amp, t_all.at[:, pl.ds(0, q_own)], load_sem.at[0])
    load("occ_tags", occ_irrep, occ_tags, load_sem.at[1])
    load("vir_tags", vir_irrep, vir_tags, load_sem.at[2])
    for k in range(width):
        load(("mate", k), slab.at[:, columns(mate, lax.rem(x + k, width))], v_mate.at[k], mate_load.at[k])
    for j in range(LINES):
        for k in others:
            load(
                ("send", j, k),
                slab.at[pl.ds(pl.multiple_of(mine * share, share), share), columns(owner[j], lax.rem(x + k, width))],
                v_send.at[j, k - 1], local_sem.at[j, k - 1],
            )
        load(("own", j), slab.at[:, columns(owner[j], x)], v_all.at[j, pl.ds(0, q_own), :], own_sem.at[j])
    load("occ_row", occ_e, occ_row, load_sem.at[3])
    load("vir_row", vir_e, vir_row, load_sem.at[4])
    load("hole", hole, hole_all, load_sem.at[5])

    pl.semaphore_wait(barrier, len(peers) - 1 + 2 * mid)

    def t_copy(i, k):
        at = some(i)
        return remote(
            t_all.at[at, pl.ds(0, q_own)], t_all.at[at, pl.ds((width - k) * q_own, q_own)],
            sent.at[0], t_sem.at[width - k - 1, i], xdev(k),
        )

    def v_piece(j, h, d, quarter):
        return v_all.at[
            j, pl.ds(pl.multiple_of(d * q_own + quarter * share, share), share), pl.ds(h * cols, cols)
        ]

    def v_copy(j, h, k):
        return remote(
            v_send.at[j, k - 1, :, pl.ds(h * cols, cols)], v_piece(j, h, width - k, mine),
            sent.at[1], v_sem.at[width - k - 1, j, h, 0], xdev(k),
        )

    def relay_copies(j, h, d, first=True, second=True):
        piece, sems = v_piece(j, h, d, mine), v_sem.at[d - 1, j, h]
        other = v_piece(j, h, d, opposite)
        copies = []
        if first:
            copies.append(remote(piece, piece, sent.at[2], sems.at[1], (across, v)))
            copies.append(remote(piece, piece, sent.at[3], sems.at[2], (partner, v)))
        if second:
            copies.append(remote(other, other, sent.at[4], sems.at[2], (partner, v)))
        return copies

    def pair_rows(oo, i):
        return cols_all.at[pl.ds(pl.multiple_of(oo * p_own + i * rows, rows), rows), :]

    def pair_copy(i, d):
        device = lax.rem(o + CORES * d, occ_size)
        return remote(
            t_all.at[pl.ds(i * rows, rows), pl.ds(0, q_own)], pair_rows(o, i), sent.at[5], pair_sem.at[groups - d - 1, i], (device, v)
        )

    def pass_copy(i, d):
        oo = lax.rem(o + CORES * d, occ_size)
        return remote(pair_rows(oo, i), pair_rows(oo, i), sent.at[6], pass_sem.at[d], (partner, v))

    fetched = set()

    def x_send(kind, n):
        for k in others:
            if kind == "t":
                t_copy(n, k).start()
                continue
            j, h = divmod(n, HALVES)
            if (j, k) not in fetched:
                fetched.add((j, k))
                loads["send", j, k].wait()
            v_copy(j, h, k).start()

    loads["amp"].wait()
    for step in ORDER:
        x_send(step[0], int(step[1:]))
        if step == "t0":
            for d in range(1, groups):
                pair_copy(0, d).start()
    own_pairs = pl.ds(pl.multiple_of(o * p_own, p_own), p_own)
    remote(t_all.at[:, pl.ds(0, q_own)], cols_all.at[own_pairs, :], sent.at[5], pass_sem.at[0], (partner, v)).start()
    load("pairs", amp, cols_all.at[pl.ds(pl.multiple_of(o * p_own, p_own), p_own), :], load_sem.at[6])

    loads["occ_tags"].wait()
    loads["vir_tags"].wait()
    low = lax.broadcasted_iota(jnp.int32, (1, 2 * TILE), 1) < TILE

    def label(ref, j, zz, xx):
        base = (zz * width + xx) * tiles

        @pl.loop(0, tiles // 2)
        def _(i):
            at = pl.ds(pl.multiple_of(i * 2 * TILE, 2 * TILE), 2 * TILE)
            ref[j, :, at] = jnp.where(low, vir_tags[base + 2 * i], vir_tags[base + 2 * i + 1])

    def pack(part):
        most = jnp.maximum(jnp.max(jnp.abs(part), axis=0, keepdims=True), 1e-30)
        return jnp.round(part * (TOP / most)).astype(jnp.int32).astype(jnp.int16), most * (1.0 / TOP)

    def early_copies(k):
        land, where = (box_in.at[0, early, :], scale_in.at[0]) if k == 0 else (early_in.at[k - 1], early_scale_in.at[k - 1])
        device = (o, mate * width + x)
        return (
            remote(early_out.at[k], land, sent.at[7], early_sem.at[0, k], device),
            remote(early_scale_out.at[k], where, sent.at[8], early_sem.at[0, k], device),
        )

    def extra_copies(k):
        return (
            remote(early_in.at[k - 1], extra_in.at[width - k - 1], sent.at[9], extra_sem.at[0, width - k - 1], xdev(k)),
            remote(
                early_scale_in.at[k - 1], extra_scale_in.at[width - k - 1],
                sent.at[10], extra_sem.at[0, width - k - 1], xdev(k),
            ),
        )

    for k in reversed(range(width)):
        label(mate_labels, k, mate, lax.rem(x + k, width))
        loads["mate", k].wait()

        @pl.loop(0, tiles)
        def _(i):
            part = pl.ds(pl.multiple_of(i * TILE, TILE), TILE)
            keep = (mate_labels[k] == vir_tags[(z * width + x) * tiles + i]).astype(jnp.float32).astype(jnp.bfloat16)
            v_mate[k, part, :] = v_mate[k, part, :] * keep

        early_out[k], early_scale_out[k] = pack(
            jnp.dot(t_all[early, pl.ds(0, q_own)], v_mate[k], preferred_element_type=jnp.float32)
        )
        for copy in early_copies(k):
            copy.start()

    for j in range(LINES):
        label(vir_labels, j, owner[j], x)

    @pl.loop(0, occ_tags.shape[0] // 2)
    def _(i):
        at = pl.ds(pl.multiple_of(i * 2 * TILE, 2 * TILE), 2 * TILE)
        occ_labels[:, at] = jnp.where(low, occ_tags[2 * i], occ_tags[2 * i + 1])

    def mask(j, d, at):
        first = (z * width + lax.rem(x + d, width)) * tiles
        labels = vir_labels[j, :, at]

        @pl.loop(0, tiles)
        def _(i):
            part = pl.ds(pl.multiple_of(d * q_own + i * TILE, TILE), TILE)
            keep = (labels == vir_tags[first + i]).astype(jnp.float32).astype(jnp.bfloat16)
            v_masked[j, part, at] = v_all[j, part, at] * keep

    everything = pl.ds(0, q_own)
    loads["own", 0].wait()
    mask(0, 0, everything)

    loads["hole"].wait()

    @pl.loop(0, p_own // TILE)
    def _(i):
        at = pl.ds(pl.multiple_of(i * TILE, TILE), TILE)
        keep = (occ_labels[...] == occ_tags[o * (p_own // TILE) + i]).astype(jnp.float32).astype(jnp.bfloat16)
        hole_all[at, :] = hole_all[at, :] * keep

    def box_copies(j, h, i):
        at, there = some(i), pl.ds(h * cols, cols)
        device = (o, target[j] * width + x)
        return (
            remote(
                box_out.at[j, at, there], box_in.at[box[j], at, there],
                sent.at[11 + j // 2], box_sem.at[box[j], h, i], device,
            ),
            remote(
                scale_out.at[j * ROWS + i, :, there], scale_in.at[box[j] * ROWS + i, :, there],
                sent.at[13 + j // 2], box_sem.at[box[j], h, i], device,
            ),
        )

    def arrived(b, h, i):
        at, there = some(i), pl.ds(h * cols, cols)
        both(starts[i + 1] - starts[i], cols, box_sem.at[b, h, i])
        return box_in[b, at, there].astype(jnp.float32) * scale_in[b * ROWS + i, :, there]

    def unit(j, h, i, merge=False):
        at, there = some(i), pl.ds(h * cols, cols)
        part = jnp.dot(t_all[at, :], v_masked[j, :, there], preferred_element_type=jnp.float32)
        if j == LINES - 1:
            acc[at, there] += part
            return
        if merge:
            part = part + arrived(j + 2, h, i)
        box_out[j, at, there], scale_out[j * ROWS + i, :, there] = pack(part)
        for copy in box_copies(j, h, i):
            copy.start()

    def skipped(j, i, inner):
        return (inner and j < LINES - 2) or (j == LINES - 2 and i < EARLY)

    def act(kind, n, i, inner, have_t, have_v):
        j, h = divmod(n, HALVES)
        if kind == "t":
            for d in others:
                landed(t_all.at[some(n), pl.ds(d * q_own, q_own)], t_sem.at[d - 1, n])
            have_t.append(n)
            for jj, hh in have_v:
                if not skipped(jj, n, inner):
                    unit(jj, hh, n)
        elif kind == "a":
            for d in others:
                landed(v_piece(j, h, d, mine), v_sem.at[d - 1, j, h, 0])
                for copy in relay_copies(j, h, d, second=False):
                    copy.start()
        elif kind == "b":
            for d in others:
                landed(v_piece(j, h, d, opposite), v_sem.at[d - 1, j, h, 1])
                relay_copies(j, h, d, first=False)[0].start()
            if h == 0 and j > 0:
                loads["own", j].wait()
                mask(j, 0, everything)
        elif kind == "c":
            for d in others:
                landed(gauge.at[pl.ds(0, 4 * share * cols // 512)], v_sem.at[d - 1, j, h, 2])
                mask(j, d, pl.ds(h * cols, cols))
            have_v.append((j, h))
            for t in have_t:
                if not skipped(j, t, inner):
                    unit(j, h, t)
        elif kind == "m":
            unit(j, h, i, merge=True)
        elif kind == "p":
            for d in range(1, groups):
                pair_copy(n, d).start()
        elif kind == "q":
            for d in range(1, groups):
                oo = lax.rem(o + CORES * d, occ_size)
                landed(pair_rows(oo, n), pair_sem.at[d - 1, n])
                pass_copy(n, d).start()
        elif kind == "e":
            for k in others:
                both(starts[EARLY], q_own, early_sem.at[0, k])
                for copy in extra_copies(k):
                    copy.start()
        elif kind == "g":
            loads["pairs"].wait()
            landed(cols_all.at[pl.ds(0, p_own), :], pass_sem.at[0])
            pairs_product(group, False)
        elif kind == "h":
            for d in range(1, groups):
                landed(cols_all.at[pl.ds(0, p_own), :], pass_sem.at[d])
                pairs_product(lax.rem(group + d, groups), True)
        else:
            loads["occ_row"].wait()
            loads["vir_row"].wait()
            for i in range(PAIR_PIECES):
                at = pl.ds(i * rows, rows)
                result[:, at] = 1.0 / (jnp.broadcast_to(vir_row[...], (rows, q_own)).T - occ_row[:, at])

    def pairs_product(g, more):
        both_cores = pl.ds(pl.multiple_of(g * CORES * p_own, CORES * p_own), CORES * p_own)

        @pl.loop(0, PAIR_PIECES)
        def _(i):
            at = pl.ds(pl.multiple_of(i * rows, rows), rows)
            part = jnp.dot(hole_all[at, both_cores], cols_all[both_cores, :], preferred_element_type=jnp.float32)
            acc[at, :] = acc[at, :] + part if more else part

    def run(actions, inner):
        have_t, have_v = [], []
        for action in actions:
            act(action[0], int(action[-1]), int(action[1]), inner, have_t, have_v)

    pl.when(mid == 0)(lambda: run(OUTER, False))
    pl.when(mid == 1)(lambda: run(INNER, True))
    for h in range(HALVES):
        for i in range(ROWS):
            acc[some(i), pl.ds(h * cols, cols)] += arrived(1, h, i)

    both(starts[EARLY], q_own, early_sem.at[0, 0])
    acc[early, :] += box_in[0, early, :].astype(jnp.float32) * scale_in[0]
    for d in others:
        both(starts[EARLY], q_own, extra_sem.at[0, d - 1])
        acc[early, :] += extra_in[d - 1].astype(jnp.float32) * extra_scale_in[d - 1]

    ends = [0] + [i + 1 for i in range(ROWS) if starts[i + 1] % LANES == 0]
    spans = list(zip(ends[:-1], ends[1:]))

    def span(first, last):
        return pl.ds(starts[first], starts[last] - starts[first])

    def out_copy(h, first, last):
        at, there = span(first, last), pl.ds(h * cols, cols)
        return pltpu.make_async_copy(result.at[there, at], out.at[there, at], out_sem.at[0])

    for h in range(HALVES):
        there = pl.ds(h * cols, cols)
        if h == HALVES - 1:
            for n, ref in enumerate((
                t_all.at[:, pl.ds(0, (width - 1) * q_own)], v_send, v_send, v_send, v_send,
                cols_all.at[pl.ds(0, groups * p_own), :], cols_all.at[pl.ds(0, (groups - 1) * p_own), :],
                early_out, early_scale_out, early_in, early_scale_in,
                box_out.at[pl.ds(0, LINES - 2)], box_out.at[LINES - 2, pl.ds(starts[EARLY], p_own - starts[EARLY]), :],
                scale_out.at[pl.ds(0, (LINES - 2) * ROWS)],
                scale_out.at[pl.ds((LINES - 2) * ROWS + EARLY, ROWS - EARLY)],
            )):
                landed(ref, sent.at[n])

        for first, last in spans:
            for i in range(max(first, EARLY), last):
                acc[some(i), there] += arrived(0, h, i)
            at = span(first, last)
            result[there, at] = acc[at, there].T * result[there, at]
            out_copy(h, first, last).start()

    landed(result, out_sem.at[0])


def per_device(
    occ_size, vir_size, amplitudes, hole_integrals, particle_integrals, occ_irrep, vir_irrep, occ_energy, vir_energy
):
    width, groups = vir_size // LINES, occ_size // CORES
    p_own, q_own = amplitudes.shape
    p_all, early = p_own * occ_size, sum(EIGHTHS[:EARLY]) * p_own // 8
    bf16, f32, i32 = jnp.bfloat16, jnp.float32, jnp.int32
    dma = pltpu.SemaphoreType.DMA
    anywhere = pl.BlockSpec(memory_space=pl.ANY)
    return pl.pallas_call(
        functools.partial(kernel, width, groups),
        out_shape=jax.ShapeDtypeStruct((q_own, p_own), f32),
        in_specs=[anywhere] * 7,
        out_specs=anywhere,
        scratch_shapes=[
            pltpu.SMEM(occ_irrep.shape, i32),
            pltpu.SMEM(vir_irrep.shape, i32),
            pltpu.VMEM((1, p_all), i32),
            pltpu.VMEM((LINES, 1, q_own), i32),
            pltpu.VMEM((1, p_own), f32),
            pltpu.VMEM((1, q_own), f32),
            pltpu.VMEM((p_own, width * q_own), bf16),
            pltpu.VMEM((LINES, width * q_own, q_own), bf16),
            pltpu.VMEM((LINES, width * q_own, q_own), bf16),
            pltpu.VMEM((LINES, width - 1, q_own // QUARTERS, q_own), bf16),
            pltpu.VMEM((width, q_own, q_own), bf16),
            pltpu.VMEM((p_all, q_own), bf16),
            pltpu.VMEM((p_own, p_all), bf16),
            pltpu.VMEM((p_own, q_own), f32),
            pltpu.VMEM((LINES - 1, p_own, q_own), jnp.int16),
            pltpu.VMEM(((LINES - 1) * ROWS, 1, q_own), f32),
            pltpu.VMEM((LINES, p_own, q_own), jnp.int16),
            pltpu.VMEM((LINES * ROWS, 1, q_own), f32),
            pltpu.VMEM((q_own, p_own), f32),
            pltpu.VMEM((width, 1, q_own), i32),
            pltpu.VMEM((width, early, q_own), jnp.int16),
            pltpu.VMEM((width, 1, q_own), f32),
            pltpu.VMEM((width - 1, early, q_own), jnp.int16),
            pltpu.VMEM((width - 1, 1, q_own), f32),
            pltpu.VMEM((width - 1, early, q_own), jnp.int16),
            pltpu.VMEM((width - 1, 1, q_own), f32),
            pltpu.VMEM(((2 * p_own * q_own + 4 * q_own) // 512, 1, LANES), f32),
            dma((15,)),
            dma((width - 1, ROWS)),
            dma((width - 1, LINES, HALVES, 3)),
            dma((groups - 1, PAIR_PIECES)),
            dma((groups,)),
            dma((LINES, HALVES, ROWS)),
            dma((LINES, width - 1)),
            dma((LINES,)),
            dma((7,)),
            dma((1,)),
            dma((width,)),
            dma((1, width)),
            dma((1, width - 1)),
        ],
        compiler_params=pltpu.CompilerParams(
            collective_id=0, has_side_effects=True, vmem_limit_bytes=60 * 1024 * 1024
        ),
    )(
        amplitudes, hole_integrals, particle_integrals, occ_irrep, vir_irrep,
        occ_energy[None, :], vir_energy[None, :],
    )


def solution(mesh):
    placed = (P("occ", "vir"), P("occ", None), P("vir", None), P(), P(), P("occ"), P("vir"))
    return jax.shard_map(
        functools.partial(per_device, mesh.shape["occ"], mesh.shape["vir"]),
        mesh=mesh, in_specs=placed, out_specs=P("vir", "occ"), check_vma=False,
    )
```
